32 devices in a mesh: gx: 4 (over z), gy: 4 (over y, x), gz: 2 (over core).
Axes of the slice: x: 2, y: 2, z: 4, core: 2. Of those that a mesh axis runs over, the one named last changes fastest.
Arguments:
- forces: float32 [3, 64, 64, 256], P(None, 'gx', 'gy', 'gz'), may hold values from -8 to 8
- mass_shift: float32 [64, 64, 256], P('gx', 'gy', 'gz'), may hold values from 0.5 to 2
- deflation: float32 [16, 3, 64, 64, 256], P(None, None, 'gx', 'gy', 'gz'), may hold values from -0.01953125 to 0.01953125
- coarse_factor: float32 [512, 512], P('gz'), may hold values from -0.041033009 to 0.6, as said below
- coarse_slot: int32 [32], replicated, may hold values from 0 to 31, each once
Outputs:
- solution: float32 [3, 64, 64, 256], P(None, 'gx', 'gy', 'gz')
- residual: float32 [3, 64, 64, 256], P(None, 'gx', 'gy', 'gz')
- direction: float32 [3, 64, 64, 256], P(None, 'gx', 'gy', 'gz')
The draws below stay inside these ranges and needn't reach their ends.
Inputs may be any that keep to these rules, and one draw needn't show every extreme that they name: `coarse_factor`: lower triangular: zero above the diagonal; diagonal entries between 0.3 and 0.6. `coarse_slot`: each subdomain has its own coarse position.
All inputs are finite; a program needn't handle non-finite values.
Results may differ from the reference program's by a relative error of at most 0.0003.
Values sent between devices are 32-bit elements; how exact they have to be, the bound alone decides.
A program may use at most 192 MiB of HBM per device.

```python
import math
import jax
import jax.numpy as jnp
from jax import lax

CX = 16
CY = 16
CZ = 128
K = 16
SWEEPS = 3
ITERS = 4
NX = 64
NY = 64
NZ = 256
SUBS = 32
NC = 512
N_GX = 4
N_GY = 4
N_GZ = 2


lower_offset = 0.012


def draw_forces(key, part):
    key_field = jax.random.fold_in(key, 3)
    along_x = (jnp.arange(NX, dtype=jnp.float32) + 0.5) / NX
    along_y = (jnp.arange(NY, dtype=jnp.float32) + 0.5) / NY
    along_z = (jnp.arange(NZ, dtype=jnp.float32) + 0.5) / NZ
    ramp_sum = along_x[:, None, None] + along_y[None, :, None] + along_z[None, None, :]
    rough_part = jax.random.truncated_normal(key_field, -4.0, 4.0, (3, NX, NY, NZ), jnp.float32)
    return rough_part * 3.0 ** (ramp_sum / 6.0)


def draw_coarse_factor(key, part):
    key_lower, key_diag = jax.random.split(jax.random.fold_in(key, 5))
    spread = 0.3 / math.sqrt(NC)
    lower_part = jax.random.truncated_normal(key_lower, -4.0, 4.0, (NC, NC), jnp.float32) * spread
    lower_part = lower_part + lower_offset
    diagonal = jax.random.uniform(key_diag, (NC,), jnp.float32, 0.3, 0.6)
    return jnp.tril(lower_part, -1) + jnp.diag(diagonal)


def level_of(key, extent, pieces, least, high):
    factor_of = 1.0
    for dim, blocks in pieces:
        steps = jax.random.uniform(jax.random.fold_in(jax.random.fold_in(key, 6), dim), (blocks,), jnp.float32, least / len(pieces), high / len(pieces))
        factor_of = factor_of * jnp.repeat(jnp.exp(steps), extent[dim] // blocks).reshape((-1,) + (1,) * (len(extent) - 1 - dim))
    return factor_of


def scatter_about(stream_key, dims, deviation, bound, cuts=(), kind=jnp.bfloat16):
    entries = deviation * jax.random.normal(stream_key, dims, jnp.float32)
    if cuts:
        entries = entries * level_of(stream_key, dims, cuts, -0.22, 0.18)
    return jnp.clip(entries, -bound, bound).astype(kind)


def setup_inputs(seed: int = 0) -> dict:
    keys = jax.random.split(jax.random.key(seed), 6)
    return {
        "forces": draw_forces(jax.random.fold_in(keys[5], 71), 0),
        "mass_shift": jnp.clip(jnp.exp(math.log(2.0) - 1.3862944 * jax.random.uniform(keys[1], (NX, NY, NZ), jnp.float32) ** level_of(keys[1], (NX, NY, NZ), ((0, 4), (1, 4), (2, 2)), -0.2, 0.2)), 0.5, 2.0),
        "deflation": scatter_about(keys[2], (K, 3, NX, NY, NZ), ((3 * CX * CY * CZ) ** -0.5), 0.01953125, ((2, 4), (3, 4), (4, 2)), jnp.float32),
        "coarse_factor": draw_coarse_factor(jax.random.fold_in(keys[5], 71), 0),
        "coarse_slot": jax.random.permutation(keys[4], SUBS).astype(jnp.int32),
    }


shear_modulus = 0.25
lame_first = 0.375
relaxation = 0.6
offsets_unit = ((1, 0, 0), (0, 1, 0), (0, 0, 1))

def stencil(padded, mass_shift):
    size_x = padded.shape[1] - 2
    size_y = padded.shape[2] - 2
    size_z = padded.shape[3] - 2
    stiffer = lame_first + shear_modulus

    def neighbor(component, shift_x, shift_y, shift_z):
        return padded[component, 1 + shift_x:1 + shift_x + size_x, 1 + shift_y:1 + shift_y + size_y, 1 + shift_z:1 + shift_z + size_z]

    def moved(component, first_unit, second_unit, sign_first, sign_second):
        return neighbor(component, sign_first * first_unit[0] + sign_second * second_unit[0], sign_first * first_unit[1] + sign_second * second_unit[1], sign_first * first_unit[2] + sign_second * second_unit[2])
    outputs = []
    for component in range(3):
        middle = neighbor(component, 0, 0, 0)
        summed = mass_shift * middle
        for axis_number in range(3):
            unit_step = offsets_unit[axis_number]
            second_diff = moved(component, unit_step, unit_step, 1, 0) + moved(component, unit_step, unit_step, -1, 0) - 2.0 * middle
            weight = shear_modulus + stiffer if axis_number == component else shear_modulus
            summed = summed - weight * second_diff
        own_unit = offsets_unit[component]
        for partner in range(3):
            if partner != component:
                partner_unit = offsets_unit[partner]
                mixed_term = moved(partner, own_unit, partner_unit, 1, 1) - moved(partner, own_unit, partner_unit, 1, -1) - moved(partner, own_unit, partner_unit, -1, 1) + moved(partner, own_unit, partner_unit, -1, -1)
                summed = summed - 0.25 * stiffer * mixed_term
        outputs.append(summed)
    return jnp.stack(outputs)

def reference(forces, mass_shift, deflation, coarse_factor, coarse_slot):
    diagonal = mass_shift + (6.0 * shear_modulus + 2.0 * (lame_first + shear_modulus))
    blocked_shape = (3, N_GX, CX, N_GY, CY, N_GZ, CZ)

    def operate(field):
        return stencil(jnp.pad(field, ((0, 0), (1, 1), (1, 1), (1, 1))), mass_shift)

    def restrict(field):
        blocked = field.reshape(blocked_shape)

        def one_vector(vector):
            return jnp.sum(vector.reshape(blocked_shape) * blocked, axis=(0, 2, 4, 6))
        sums = lax.map(one_vector, deflation)
        return jnp.transpose(sums, (1, 2, 3, 0)).reshape(N_GX * N_GY * N_GZ, K)

    def prolong(weights):
        grid = jnp.transpose(weights.reshape(N_GX, N_GY, N_GZ, K), (3, 0, 1, 2))

        def add_vector(summed, pair):
            vector, scales = pair
            return (summed + vector.reshape(blocked_shape) * scales[None, :, None, :, None, :, None], None)
        start = jnp.zeros(blocked_shape, jnp.float32)
        summed, ignored = lax.scan(add_vector, start, (deflation, grid))
        return summed.reshape(3, NX, NY, NZ)

    def precondition(field):
        restricted = restrict(field)
        ordered = jnp.zeros_like(restricted).at[coarse_slot].set(restricted).reshape(-1)
        forward = jax.scipy.linalg.solve_triangular(coarse_factor, ordered, lower=True)
        coarse = jax.scipy.linalg.solve_triangular(coarse_factor, forward, lower=True, trans=1)
        correction = prolong(coarse.reshape(-1, K)[coarse_slot])
        smooth = jnp.zeros_like(field)
        for sweep_index in range(SWEEPS):
            smooth = smooth + relaxation * (field - operate(smooth)) / diagonal
        return correction + smooth
    solution = jnp.zeros_like(forces)
    residual = forces
    direction = forces
    precond_prior = jnp.float32(1.0)
    for iteration in range(ITERS):
        preconditioned = precondition(residual)
        precond_norm = jnp.sum(residual * preconditioned)
        if iteration == 0:
            direction = preconditioned
        else:
            direction = preconditioned + precond_norm / precond_prior * direction
        image_field = operate(direction)
        step_size = precond_norm / jnp.sum(direction * image_field)
        solution = solution + step_size * direction
        residual = residual - step_size * image_field
        precond_prior = precond_norm
    return (solution, residual, direction)
```

```python
import functools

import jax
import jax.numpy as jnp
from jax import lax
from jax.experimental import pallas as pl
from jax.experimental.pallas import tpu as pltpu
from jax.sharding import PartitionSpec as P

SWEEPS = 3
ITERS = 4
MESH = pl.DeviceIdType.MESH
HIGHEST = lax.Precision.HIGHEST
W = SWEEPS
DIRS = ((0, -1), (0, 1), (-1, 0), (1, 0), (-1, -1), (-1, 1), (1, -1), (1, 1))
BLOCK = 128


def dot(a, b):
    return jnp.dot(a, b, precision=HIGHEST, preferred_element_type=jnp.float32)


def up8(v):
    return -(-v // 8) * 8


def kernel(
    sizes,
    forces, mass, defl_hbm, factor, slots_hbm,
    sol, res, direc,
    zext, rext, idir, cext, cquarter, mext, cor, ua, ub, uz,
    zsend, zgot, edge, fix, cpack, defl,
    full, inv, sol_mat, turned, krows, gsend, gat, gres, gdir, slots,
    zx_send, zx_recv, c_send, c_recv, m_send, m_recv,
    zc_send, zc_recv, g_send, g_recv, f_send, f_recv, i_send, i_recv, local,
):
    nx, ny, nz, cx, cy, vectors, order = sizes
    n = nx * ny * nz
    ex = cx + 2 * W
    pitch = zext.shape[3]
    tall = up8(cy + 2 * W)
    gx, gy, gz = lax.axis_index("gx"), lax.axis_index("gy"), lax.axis_index("gz")
    me = (gx * ny + gy) * nz + gz
    f32 = jnp.float32

    def wrap(a, d, size):
        s = a + d
        return jnp.where(s >= size, s - size, s)

    others = [
        {"gx": wrap(gx, dx, nx), "gy": wrap(gy, dy, ny), "gz": wrap(gz, dz, nz)}
        for dx in range(nx) for dy in range(ny) for dz in range(nz) if (dx, dy, dz) != (0, 0, 0)
    ]
    own_x, own_y = pl.ds(W, cx), pl.ds(W, cy)
    load_factor = pltpu.make_async_copy(factor, full.at[gz], local.at[0])
    load_factor.start()
    load_slots = pltpu.make_async_copy(slots_hbm, slots, local.at[1])
    load_slots.start()

    def clear(ref):
        lead = ref.shape[0]
        zero = jnp.zeros(ref.shape[2:], f32)

        def one(i, _):
            for c in range(lead):
                ref[c, i] = zero
            return 0

        lax.fori_loop(0, ref.shape[1], one, 0)

    for ref in (zext.at[0], zext.at[1], mext, cor):
        clear(ref)
    zgot[...] = jnp.zeros(zgot.shape, f32)
    barrier = pltpu.get_barrier_semaphore()
    for other in others:
        pl.semaphore_signal(barrier, inc=1, device_id=other, device_id_type=MESH)
    load_forces = pltpu.make_async_copy(forces, zext.at[0, :, own_x, own_y], local.at[2])
    load_forces.start()
    load_mass = pltpu.make_async_copy(mass, mext.at[0, own_x, own_y], local.at[3])
    load_mass.start()
    load_defl = pltpu.make_async_copy(defl_hbm, defl, local.at[4])
    load_defl.start()
    for ref in (ua, ub, uz):
        clear(ref)
    for ref in (zsend, edge, fix, cpack):
        ref[...] = jnp.zeros(ref.shape, f32)

    lane = lax.broadcasted_iota(jnp.int32, (tall, 128), 1)
    lane8 = lax.broadcasted_iota(jnp.int32, (8, 128), 1)
    row8 = lax.broadcasted_iota(jnp.int32, (8, 128), 0)
    lane1 = lax.broadcasted_iota(jnp.int32, (1, 128), 1)
    rim = (lane == 0) | (lane == 127)
    rim_own = (lax.broadcasted_iota(jnp.int32, (cy, 128), 1) + 1) % 128 < 2
    even = lane % 2 == 0
    sign = jnp.where(even, 0.15625, -0.15625)
    base = (me % 8) * vectors

    slab = order // nz
    per_slab = slab // BLOCK
    blocks = order // BLOCK
    r_i = lax.broadcasted_iota(jnp.int32, (BLOCK, BLOCK), 0)
    c_i = lax.broadcasted_iota(jnp.int32, (BLOCK, BLOCK), 1)
    load_factor.wait()
    lows, xs = [], []
    for q in range(per_slab):
        col = pl.ds(pl.multiple_of((gz * per_slab + q) * BLOCK, BLOCK), BLOCK)
        block = full[gz, q * BLOCK : (q + 1) * BLOCK, col]
        lows.append(block)
        xs.append(jnp.where(r_i == c_i, 1.0 / jnp.where(r_i == c_i, block, 1.0), 0.0))
    s = 1
    while s < BLOCK:
        pick = (r_i // (2 * s) == c_i // (2 * s)) & ((r_i // s) % 2 == 1) & ((c_i // s) % 2 == 0)
        mids = [dot(jnp.where(pick, lows[q], 0.0), xs[q]) for q in range(per_slab)]
        xs = [xs[q] - dot(xs[q], mids[q]) for q in range(per_slab)]
        s *= 2
    for q in range(per_slab):
        inv[gz * per_slab + q] = xs[q]

    def slab_copies(j):
        t = wrap(gz, j, nz)
        to = {"gx": gx, "gy": gy, "gz": t}
        mine = pl.ds(gz * per_slab, per_slab)
        return (
            pltpu.make_async_remote_copy(
                src_ref=full.at[gz], dst_ref=full.at[gz], send_sem=f_send.at[j - 1],
                recv_sem=f_recv.at[j - 1], device_id=to, device_id_type=MESH,
            ),
            pltpu.make_async_remote_copy(
                src_ref=inv.at[mine], dst_ref=inv.at[mine], send_sem=i_send.at[j - 1],
                recv_sem=i_recv.at[j - 1], device_id=to, device_id_type=MESH,
            ),
        )

    def exists(dx, dy):
        ok = jnp.bool_(True)
        if dx < 0:
            ok = jnp.logical_and(ok, gx > 0)
        if dx > 0:
            ok = jnp.logical_and(ok, gx < nx - 1)
        if dy < 0:
            ok = jnp.logical_and(ok, gy > 0)
        if dy > 0:
            ok = jnp.logical_and(ok, gy < ny - 1)
        return ok

    def span(d, size, width):
        if d == 0:
            return pl.ds(W, size), pl.ds(W, size)
        if d < 0:
            return pl.ds(W, width), pl.ds(W + size, width)
        return pl.ds(W + size - width, width), pl.ds(W - width, width)

    def pieces(ext, width, send, recv):
        out = []
        for d, (dx, dy) in enumerate(DIRS):
            sx, tx = span(dx, cx, width)
            sy, ty = span(dy, cy, width)
            copy = pltpu.make_async_remote_copy(
                src_ref=ext.at[:, sx, sy],
                dst_ref=ext.at[:, tx, ty],
                send_sem=send.at[d],
                recv_sem=recv.at[d],
                device_id={"gx": gx + dx, "gy": gy + dy, "gz": gz},
                device_id_type=MESH,
            )
            out.append((dx, dy, copy))
        return out

    def send_halo(*args):
        for dx, dy, copy in pieces(*args):
            pl.when(exists(dx, dy))(copy.start)

    def take_halo(*args):
        for dx, dy, copy in pieces(*args):
            pl.when(exists(-dx, -dy))(copy.wait_recv)
            pl.when(exists(dx, dy))(copy.wait_send)

    def halo_z(slot):
        return zext.at[slot], W, zx_send, zx_recv.at[slot]

    halo_m = (mext, W, m_send, m_recv)
    thin = (cor, 1, c_send, c_recv)

    has = (gz > 0, gz < nz - 1)

    def columns(stage, side):
        return pltpu.make_async_remote_copy(
            src_ref=zsend.at[stage],
            dst_ref=zgot.at[stage, 1 - side],
            send_sem=zc_send.at[stage, side],
            recv_sem=zc_recv.at[stage, side],
            device_id={"gx": gx, "gy": gy, "gz": gz + (2 * side - 1)},
            device_id_type=MESH,
        )

    def gathered(v, x, acc):
        return jnp.where(lane // 2 == x, pltpu.roll(v, 2 * x + 1, 1), acc)

    nothing = (jnp.zeros((tall, 128), f32),) * 3

    def send_columns(stage, first, acc):
        for c in range(3):
            swapped = jnp.where(even, pltpu.roll(acc[c], 127, 1), pltpu.roll(acc[c], 1, 1))
            zsend[stage, c, first : first + tall] = swapped
        for side in (0, 1):
            pl.when(has[side])(columns(stage, side).start)

    def take_columns(stage, first, scaled):
        for side in (0, 1):
            pl.when(has[1 - side])(columns(stage, side).wait_recv)
            pl.when(has[side])(columns(stage, side).wait_send)
        e = []
        for c in range(3):
            v = jnp.where(
                even, zgot[stage, 1, c, first - 1 : first - 1 + tall], zgot[stage, 0, c, first - 1 : first - 1 + tall]
            ) - zsend[stage, c, first - 1 : first - 1 + tall]
            edge[c, first - 1 : first - 1 + tall] = v

        def at(c, dy):
            return edge[c, first + dy : first + dy + tall]

        def along(v):
            return pltpu.roll(v, 126, 1) - pltpu.roll(v, 2, 1)

        ex_, ey_, ez_ = at(0, 0), at(1, 0), at(2, 0)
        fx = 0.25 * ex_ + sign * along(ez_)
        fy = 0.25 * ey_ + sign * (at(2, 1) - at(2, -1))
        fz = 0.875 * ez_ + sign * (along(ex_) + (at(1, 1) - at(1, -1)))
        for c, f in enumerate((fx, fy, fz)):
            fix[c, first : first + tall] = cpack[first : first + tall] * f if scaled else f

    def stencil(u, x, r):
        def at(c, dx, dy):
            return u[c, x + dx, r + dy : r + dy + 8]

        def z_diff(v):
            return pltpu.roll(v, 127, 1) - pltpu.roll(v, 1, 1)

        here = [at(c, 0, 0) for c in range(3)]
        xp, xm = [at(c, 1, 0) for c in range(3)], [at(c, -1, 0) for c in range(3)]
        yp, ym = [at(c, 0, 1) for c in range(3)], [at(c, 0, -1) for c in range(3)]
        sx = [xp[c] + xm[c] for c in range(3)]
        sy = [yp[c] + ym[c] for c in range(3)]
        sz = [pltpu.roll(here[c], 127, 1) + pltpu.roll(here[c], 1, 1) for c in range(3)]
        mx = (at(1, 1, 1) - at(1, 1, -1)) - (at(1, -1, 1) - at(1, -1, -1)) + z_diff(xp[2] - xm[2])
        my = (at(0, 1, 1) - at(0, -1, 1)) - (at(0, 1, -1) - at(0, -1, -1)) + z_diff(yp[2] - ym[2])
        mz = z_diff((xp[0] - xm[0]) + (yp[1] - ym[1]))
        t = (
            (sy[0] + sz[0]) + 3.5 * sx[0] + 0.625 * mx,
            (sx[1] + sz[1]) + 3.5 * sy[1] + 0.625 * my,
            (sx[2] + sy[2]) + 3.5 * sz[2] + 0.625 * mz,
        )
        return here, t

    def sweep(src, dst, depth):
        first = W - depth
        rows = up8(cy + 2 * depth)

        def at(x, _):
            for r in range(first, first + rows, 8):
                here, t = stencil(src, x, r)
                q = cquarter[x, r : r + 8]
                for c in range(3):
                    if src is ua:
                        dst[c, x, r : r + 8] = 1.4 * here[c] + q * t[c]
                    else:
                        dst[c, x, r : r + 8] = 0.4 * here[c] + (ua[c, x, r : r + 8] + q * t[c])
            return 0

        lax.fori_loop(first, W + cx + depth, at, 0)

    def mend(u, depth, extra):
        first = W - depth
        part = slice(first, first + tall)

        def at(x, acc):
            out = []
            for c in range(3):
                v = u[c, x, part] + jnp.where(rim, pltpu.roll(fix[c, part], 127 - 2 * x, 1), 0.0)
                if extra is not None:
                    v = v + extra[c, x, part]
                u[c, x, part] = v
                out.append(gathered(v, x, acc[c]))
            return tuple(out)

        return lax.fori_loop(first, W + cx + depth, at, nothing)

    def push(slot, acc, gamma, energy):
        line = jnp.zeros((1, 128), f32)
        for k in range(vectors):
            total = jnp.sum(jnp.sum(acc[k], axis=0, keepdims=True), axis=1, keepdims=True)
            line = jnp.where(lane1 == base + k, total, line)
        if gamma is not None:
            line = jnp.where(lane1 == (base + vectors) % 128, gamma, line)
            line = jnp.where(lane1 == (base + vectors + 1) % 128, energy, line)
        gsend[slot, 0:1] = line
        gat[slot, pl.ds(me, 1)] = line
        for other in others:
            pltpu.make_async_remote_copy(
                src_ref=gsend.at[slot, 0],
                dst_ref=gat.at[slot, me],
                send_sem=g_send.at[slot],
                recv_sem=g_recv.at[slot],
                device_id=other,
                device_id_type=MESH,
            ).start()

    def collect(slot):
        rest = gat.at[slot, pl.ds(0, n - 1)]
        pltpu.make_async_copy(rest, rest, g_recv.at[slot]).wait()
        pltpu.make_async_copy(rest, rest, g_send.at[slot]).wait()
        lines, both = [], jnp.zeros((8, 128), f32)
        for t in range(n // 8):
            tile = gat[slot, 8 * t : 8 * t + 8]
            lines.append(jnp.sum(jnp.where(lane8 // vectors == row8, tile, 0.0), axis=0, keepdims=True))
            both = both + tile
        g_at = (row8 * vectors + vectors) % 128
        gamma = jnp.sum(jnp.where(lane8 == g_at, both, 0.0), axis=0, keepdims=True)
        energy = jnp.sum(jnp.where(lane8 == g_at + 1, both, 0.0), axis=0, keepdims=True)
        return lines, jnp.sum(gamma, axis=1, keepdims=True), jnp.sum(energy, axis=1, keepdims=True)

    def restrict(x, values, acc):
        acc = list(acc)
        for c in range(3):
            for k in range(vectors):
                prod = defl[k, c, x] * values[c]
                for t in range(0, cy, 8):
                    acc[k] = acc[k] + prod[t : t + 8]
        return acc

    clean = (jnp.zeros((8, 128), f32),) * vectors
    load_forces.wait()
    load_defl.wait()

    def first_share(x, acc):
        return tuple(restrict(x, [zext[0, c, W + x, W : W + cy] for c in range(3)], acc))

    acc = lax.fori_loop(0, cx, first_share, clean)
    load_mass.wait()

    pl.semaphore_wait(barrier, n - 1)
    push(0, acc, None, None)
    for j in range(1, nz):
        for copy in slab_copies(j):
            copy.start()
    send_halo(*halo_z(0))
    send_halo(*halo_m)

    load_slots.wait()
    for j in range(1, nz):
        for copy in slab_copies(j):
            copy.wait_recv()
            copy.wait_send()

    width = min(512, order)
    w_rows = lax.broadcasted_iota(jnp.int32, (BLOCK, width), 0)

    def slot_line(t):
        line = jnp.zeros((1, 128), jnp.int32)
        for r in range(8):
            line = jnp.where(lane1 // vectors == r, slots[8 * t + r] * vectors + lane1 % vectors, line)
        return line

    def one_hot(i, j):
        line = jnp.concatenate([slot_line(j * (width // 128) + t) for t in range(width // 128)], axis=1)
        return jnp.where(w_rows + i * BLOCK == line, 1.0, 0.0)

    if blocks <= 4:
        for i in range(blocks):
            right = one_hot(i, 0)
            if i:
                at = slice((i % per_slab) * BLOCK, (i % per_slab + 1) * BLOCK)
                right = right - dot(full[i // per_slab, at, 0 : i * BLOCK], sol_mat[0 : i * BLOCK])
            sol_mat[i * BLOCK : (i + 1) * BLOCK] = dot(inv[i], right)
    else:
        def wipe(i, _):
            sol_mat[pl.ds(pl.multiple_of(i * 8, 8), 8), :] = jnp.zeros((8, order), f32)
            return 0

        lax.fori_loop(0, order // 8, wipe, 0)

        def substitute(i, _):
            at = pl.ds(pl.multiple_of((i % per_slab) * BLOCK, BLOCK), BLOCK)
            for j in range(order // width):
                col = slice(j * width, (j + 1) * width)
                right = one_hot(i, j) - dot(full[i // per_slab, at, :], sol_mat[:, col])
                sol_mat[pl.ds(pl.multiple_of(i * BLOCK, BLOCK), BLOCK), col] = dot(inv[i], right)
            return 0

        lax.fori_loop(0, blocks, substitute, 0)

    mine = pl.ds(pl.multiple_of((me // 8) * 128, 128), 128)

    def turn(i, _):
        at = pl.ds(pl.multiple_of(i * BLOCK, BLOCK), BLOCK)
        turned[:, at] = sol_mat[at, mine].T
        return 0

    lax.fori_loop(0, blocks, turn, 0)
    own_rows = pl.ds(pl.multiple_of(base, 8), vectors)

    def form(j, _):
        col = pl.ds(pl.multiple_of(j * width, width), width)
        krows[:, col] = dot(turned[own_rows, :], sol_mat[:, col])
        return 0

    lax.fori_loop(0, order // width, form, 0)

    def coarse():
        y = jnp.zeros((vectors, 128), f32)
        for t in range(order // 128):
            y = y + krows[:, t * 128 : (t + 1) * 128] * gres[t]
        y = jnp.broadcast_to(jnp.sum(y, axis=1, keepdims=True), (vectors, 128))
        spread = [jnp.broadcast_to(y[k : k + 1], (8, 128)) for k in range(vectors)]

        def correct(x, _):
            for c in range(3):
                for t in range(0, cy, 8):
                    acc = spread[0] * defl[0, c, x, t : t + 8]
                    for k in range(1, vectors):
                        acc = acc + spread[k] * defl[k, c, x, t : t + 8]
                    cor[c, W + x, W + t : W + t + 8] = acc
            return 0

        lax.fori_loop(0, cx, correct, 0)

    lines, _, _ = collect(0)
    for t in range(n // 8):
        gres[t] = lines[t]
        gdir[t] = jnp.zeros((1, 128), f32)
    coarse()
    send_halo(*thin)
    take_halo(*halo_z(0))
    take_halo(*halo_m)
    rows = lax.broadcasted_iota(jnp.int32, (pitch, 128), 0)
    y_ok = ((rows >= W) | (gy > 0)) & ((rows < W + cy) | (gy < ny - 1)) & (rows < cy + 2 * W)

    def settle(x, acc):
        x_ok = ((x >= W) | (gx > 0)) & ((x < W + cx) | (gx < nx - 1))
        keep = jnp.where(x_ok, 1.0, 0.0)
        v = jnp.where(y_ok, 0.6 / (mext[0, x] + 2.75), 0.0) * keep
        cext[x] = v
        cquarter[x] = 0.25 * v
        out = [gathered(v[0:tall], x, acc[3])]
        new = []
        for c in range(3):
            f = zext[0, c, x]
            rext[c, x] = f
            idir[c, x] = jnp.zeros((pitch, 128), f32)
            u = v[0:tall] * f[0:tall]
            ua[c, x, 0:tall] = u
            new.append(gathered(u, x, acc[c]))
        return tuple(new) + tuple(out)

    acc = lax.fori_loop(0, ex, settle, nothing + (nothing[0],))
    cpack[0:tall] = acc[3]
    send_columns(0, 0, acc[0:3])

    def own_clear(x, _):
        for c in range(3):
            sol[c, x] = jnp.zeros((cy, 128), f32)
            direc[c, x] = jnp.zeros((cy, 128), f32)
        return 0

    lax.fori_loop(0, cx, own_clear, 0)

    def iterate(it, carry):
        gamma_prior, step_prior = carry
        slot = (it + 1) % 2
        sweep(ua, ub, 2)
        take_columns(0, 1, True)
        acc = mend(ub, 2, None)
        send_columns(1, 1, acc)
        sweep(ub, uz, 1)
        take_columns(1, 2, True)
        take_halo(*thin)
        acc = mend(uz, 1, cor)
        send_columns(2, 2, acc)

        def image(x, _):
            for t in range(0, cy, 8):
                here, off = stencil(uz, x, W + t)
                diag = mext[0, x, W + t : W + t + 8] + 2.75
                for c in range(3):
                    zext[slot, c, x, W + t : W + t + 8] = diag * here[c] - 0.25 * off[c]
            return 0

        lax.fori_loop(W, W + cx, image, 0)
        take_columns(2, 3, False)

        def finish(x, carry):
            gam, ene, acc = carry[0], carry[1], carry[2:]
            values = []
            for c in range(3):
                f = pltpu.roll(fix[c, W : W + cy], 127 - 2 * W - 2 * x, 1)
                a = zext[slot, c, W + x, W : W + cy] - jnp.where(rim_own, f, 0.0)
                zext[slot, c, W + x, W : W + cy] = a
                z = uz[c, W + x, W : W + cy]
                gam = gam + rext[c, W + x, W : W + cy] * z
                ene = ene + z * a
                values.append(a)
            return (gam, ene) + tuple(restrict(x, values, acc))

        blank = jnp.zeros((cy, 128), f32)
        carry = lax.fori_loop(0, cx, finish, (blank, blank) + clean)
        gam = jnp.sum(jnp.sum(carry[0], axis=0, keepdims=True), axis=1, keepdims=True)
        ene = jnp.sum(jnp.sum(carry[1], axis=0, keepdims=True), axis=1, keepdims=True)
        push(slot, carry[2:], gam, ene)

        @pl.when(it < ITERS - 1)
        def _():
            send_halo(*halo_z(slot))

        lines, gamma, energy = collect(slot)
        momentum = jnp.where(it == 0, 0.0, gamma / gamma_prior)
        step = gamma / (energy - momentum * gamma / step_prior)

        @pl.when(it < ITERS - 1)
        def _():
            for t in range(n // 8):
                image_line = lines[t] + momentum * gdir[t]
                gdir[t] = image_line
                gres[t] = gres[t] - step * image_line
            coarse()
            send_halo(*thin)
            take_halo(*halo_z(slot))

            def update(x, acc):
                out = []
                for c in range(3):
                    image_dir = zext[slot, c, x, 0:tall] + momentum * idir[c, x, 0:tall]
                    idir[c, x, 0:tall] = image_dir
                    r = rext[c, x, 0:tall] - step * image_dir
                    rext[c, x, 0:tall] = r
                    u = cext[x, 0:tall] * r
                    ua[c, x, 0:tall] = u
                    out.append(gathered(u, x, acc[c]))
                return tuple(out)

            acc = lax.fori_loop(0, ex, update, nothing)
            send_columns(0, 0, acc)

        def advance(x, _):
            for c in range(3):
                d = uz[c, W + x, W : W + cy] + momentum * direc[c, x]
                direc[c, x] = d
                sol[c, x] = sol[c, x] + step * d
            return 0

        lax.fori_loop(0, cx, advance, 0)

        @pl.when(it == ITERS - 1)
        def _():
            def give(x, _):
                for c in range(3):
                    image_dir = zext[slot, c, W + x, W : W + cy] + momentum * idir[c, W + x, W : W + cy]
                    res[c, x] = rext[c, W + x, W : W + cy] - step * image_dir
                return 0

            lax.fori_loop(0, cx, give, 0)

        return gamma, step

    one = jnp.ones((1, 1), f32)
    lax.fori_loop(0, ITERS, iterate, (one, one))


def solution(mesh):
    nx, ny, nz = mesh.shape["gx"], mesh.shape["gy"], mesh.shape["gz"]

    def body(forces, mass_shift, deflation, coarse_factor, coarse_slot):
        vectors = deflation.shape[0]
        cx, cy = forces.shape[1], forces.shape[2]
        order = coarse_factor.shape[1]
        slab = coarse_factor.shape[0]
        n = nx * ny * nz
        ex, pitch = cx + 2 * W, up8(up8(cy + 2 * W) + W)
        f32 = jnp.float32
        vm = lambda *shape: pltpu.VMEM(shape, f32)
        field = (3, ex, pitch, 128)
        dma = pltpu.SemaphoreType.DMA
        peers = max(nz - 1, 1)
        return pl.pallas_call(
            functools.partial(kernel, (nx, ny, nz, cx, cy, vectors, order)),
            out_shape=[jax.ShapeDtypeStruct(forces.shape, f32)] * 3,
            in_specs=[pl.BlockSpec(memory_space=pl.ANY)] * 5,
            out_specs=[pl.BlockSpec(memory_space=pltpu.VMEM)] * 3,
            scratch_shapes=[
                vm(2, *field), vm(*field), vm(*field), vm(ex, pitch, 128), vm(ex, pitch, 128),
                vm(1, ex, pitch, 128), vm(*field), vm(*field), vm(*field), vm(*field),
                vm(3, 3, pitch, 128), vm(3, 2, 3, pitch, 128), vm(3, pitch, 128), vm(3, pitch, 128),
                vm(pitch, 128), vm(*deflation.shape),
                vm(nz, slab, order), vm(order // BLOCK, BLOCK, BLOCK), vm(order, order),
                vm(BLOCK, order), vm(vectors, order),
                vm(2, 8, 128), vm(2, n, 128), vm(n // 8, 1, 128), vm(n // 8, 1, 128),
                pltpu.SMEM(coarse_slot.shape, jnp.int32),
                dma((8,)), dma((2, 8)), dma((8,)), dma((8,)), dma((8,)), dma((8,)),
                dma((3, 2)), dma((3, 2)), dma((2,)), dma((2,)),
                dma((peers,)), dma((peers,)), dma((peers,)), dma((peers,)), dma((5,)),
            ],
            compiler_params=pltpu.CompilerParams(
                collective_id=0, has_side_effects=True, vmem_limit_bytes=66 * 1000 * 1000
            ),
        )(forces, mass_shift, deflation, coarse_factor, coarse_slot)

    return jax.shard_map(
        body,
        mesh=mesh,
        in_specs=(
            P(None, "gx", "gy", "gz"),
            P("gx", "gy", "gz"),
            P(None, None, "gx", "gy", "gz"),
            P("gz", None),
            P(),
        ),
        out_specs=(P(None, "gx", "gy", "gz"), P(None, "gx", "gy", "gz"), P(None, "gx", "gy", "gz")),
        check_vma=False,
    )
```

```python
import functools

import jax
import jax.numpy as jnp
from jax import lax
from jax.experimental import pallas as pl
from jax.experimental.pallas import tpu as pltpu
from jax.sharding import PartitionSpec as P

SWEEPS = 3
ITERS = 4
MESH = pl.DeviceIdType.MESH
HIGHEST = lax.Precision.HIGHEST
W = SWEEPS
DIRS = ((0, -1), (0, 1), (-1, 0), (1, 0), (-1, -1), (-1, 1), (1, -1), (1, 1))
BLOCK = 128


def dot(a, b):
    return jnp.dot(a, b, precision=HIGHEST, preferred_element_type=jnp.float32)


def up8(v):
    return -(-v // 8) * 8


def planes(first, last, body, carry, most):
    count = last - first
    step = max(d for d in range(1, most + 1) if count % d == 0)

    def some(i, carry):
        for j in range(step):
            carry = body(first + i * step + j, carry)
        return carry

    return lax.fori_loop(0, count // step, some, carry)


def kernel(
    sizes,
    forces, mass, defl_hbm, factor, slots_hbm,
    sol, res, direc,
    zext, rext, idir, cext, cquarter, mext, cor, ua, ub, uz,
    zsend, zgot, edge, fix, cpack, defl,
    full, inv, sol_mat, turned, krows, gsend, gat, gres, gdir, slots,
    zx_send, zx_recv, c_send, c_recv, m_send, m_recv,
    zc_send, zc_recv, g_send, g_recv, f_send, f_recv, i_send, i_recv, local,
):
    nx, ny, nz, cx, cy, vectors, order = sizes
    n = nx * ny * nz
    ex = cx + 2 * W
    pitch = zext.shape[3]
    tall = up8(cy + 2 * W)
    gx, gy, gz = lax.axis_index("gx"), lax.axis_index("gy"), lax.axis_index("gz")
    me = (gx * ny + gy) * nz + gz
    f32 = jnp.float32

    def wrap(a, d, size):
        s = a + d
        return jnp.where(s >= size, s - size, s)

    others = [
        {"gx": wrap(gx, dx, nx), "gy": wrap(gy, dy, ny), "gz": wrap(gz, dz, nz)}
        for dx in range(nx) for dy in range(ny) for dz in range(nz) if (dx, dy, dz) != (0, 0, 0)
    ]
    own_x, own_y = pl.ds(W, cx), pl.ds(W, cy)
    load_factor = pltpu.make_async_copy(factor, full.at[gz], local.at[0])
    load_factor.start()
    load_slots = pltpu.make_async_copy(slots_hbm, slots, local.at[1])
    load_slots.start()

    def clear(ref):
        lead = ref.shape[0]
        zero = jnp.zeros(ref.shape[2:], f32)

        def one(i, _):
            for c in range(lead):
                ref[c, i] = zero
            return 0

        lax.fori_loop(0, ref.shape[1], one, 0)

    for ref in (zext.at[0], zext.at[1], mext, cor):
        clear(ref)
    zgot[...] = jnp.zeros(zgot.shape, f32)
    barrier = pltpu.get_barrier_semaphore()
    for other in others:
        pl.semaphore_signal(barrier, inc=1, device_id=other, device_id_type=MESH)
    load_forces = pltpu.make_async_copy(forces, zext.at[0, :, own_x, own_y], local.at[2])
    load_forces.start()
    load_mass = pltpu.make_async_copy(mass, mext.at[0, own_x, own_y], local.at[3])
    load_mass.start()
    load_defl = pltpu.make_async_copy(defl_hbm, defl, local.at[4])
    load_defl.start()
    for ref in (ua, ub, uz):
        clear(ref)
    for ref in (zsend, edge, fix, cpack):
        ref[...] = jnp.zeros(ref.shape, f32)

    lane = lax.broadcasted_iota(jnp.int32, (tall, 128), 1)
    lane8 = lax.broadcasted_iota(jnp.int32, (8, 128), 1)
    row8 = lax.broadcasted_iota(jnp.int32, (8, 128), 0)
    lane1 = lax.broadcasted_iota(jnp.int32, (1, 128), 1)
    rim = (lane == 0) | (lane == 127)
    rim_own = (lax.broadcasted_iota(jnp.int32, (cy, 128), 1) + 1) % 128 < 2
    even = lane % 2 == 0
    sign = jnp.where(even, 0.15625, -0.15625)
    base = (me % 8) * vectors

    slab = order // nz
    per_slab = slab // BLOCK
    blocks = order // BLOCK
    r_i = lax.broadcasted_iota(jnp.int32, (BLOCK, BLOCK), 0)
    c_i = lax.broadcasted_iota(jnp.int32, (BLOCK, BLOCK), 1)
    load_factor.wait()
    lows, xs = [], []
    for q in range(per_slab):
        col = pl.ds(pl.multiple_of((gz * per_slab + q) * BLOCK, BLOCK), BLOCK)
        block = full[gz, q * BLOCK : (q + 1) * BLOCK, col]
        lows.append(block)
        xs.append(jnp.where(r_i == c_i, 1.0 / jnp.where(r_i == c_i, block, 1.0), 0.0))
    s = 1
    while s < BLOCK:
        pick = (r_i // (2 * s) == c_i // (2 * s)) & ((r_i // s) % 2 == 1) & ((c_i // s) % 2 == 0)
        mids = [dot(jnp.where(pick, lows[q], 0.0), xs[q]) for q in range(per_slab)]
        xs = [xs[q] - dot(xs[q], mids[q]) for q in range(per_slab)]
        s *= 2
    for q in range(per_slab):
        inv[gz * per_slab + q] = xs[q]

    def slab_copies(j):
        t = wrap(gz, j, nz)
        to = {"gx": gx, "gy": gy, "gz": t}
        mine = pl.ds(gz * per_slab, per_slab)
        return (
            pltpu.make_async_remote_copy(
                src_ref=full.at[gz], dst_ref=full.at[gz], send_sem=f_send.at[j - 1],
                recv_sem=f_recv.at[j - 1], device_id=to, device_id_type=MESH,
            ),
            pltpu.make_async_remote_copy(
                src_ref=inv.at[mine], dst_ref=inv.at[mine], send_sem=i_send.at[j - 1],
                recv_sem=i_recv.at[j - 1], device_id=to, device_id_type=MESH,
            ),
        )

    def exists(dx, dy):
        ok = jnp.bool_(True)
        if dx < 0:
            ok = jnp.logical_and(ok, gx > 0)
        if dx > 0:
            ok = jnp.logical_and(ok, gx < nx - 1)
        if dy < 0:
            ok = jnp.logical_and(ok, gy > 0)
        if dy > 0:
            ok = jnp.logical_and(ok, gy < ny - 1)
        return ok

    def span(d, size, width):
        if d == 0:
            return pl.ds(W, size), pl.ds(W, size)
        if d < 0:
            return pl.ds(W, width), pl.ds(W + size, width)
        return pl.ds(W + size - width, width), pl.ds(W - width, width)

    def pieces(ext, width, send, recv):
        out = []
        for d, (dx, dy) in enumerate(DIRS):
            sx, tx = span(dx, cx, width)
            sy, ty = span(dy, cy, width)
            copy = pltpu.make_async_remote_copy(
                src_ref=ext.at[:, sx, sy],
                dst_ref=ext.at[:, tx, ty],
                send_sem=send.at[d],
                recv_sem=recv.at[d],
                device_id={"gx": gx + dx, "gy": gy + dy, "gz": gz},
                device_id_type=MESH,
            )
            out.append((dx, dy, copy))
        return out

    def send_halo(*args):
        for dx, dy, copy in pieces(*args):
            pl.when(exists(dx, dy))(copy.start)

    def take_halo(*args):
        for dx, dy, copy in pieces(*args):
            pl.when(exists(-dx, -dy))(copy.wait_recv)
            pl.when(exists(dx, dy))(copy.wait_send)

    def halo_z(slot):
        return zext.at[slot], W, zx_send, zx_recv.at[slot]

    halo_m = (mext, W, m_send, m_recv)
    thin = (cor, 1, c_send, c_recv)

    has = (gz > 0, gz < nz - 1)

    def columns(stage, side):
        return pltpu.make_async_remote_copy(
            src_ref=zsend.at[stage],
            dst_ref=zgot.at[stage, 1 - side],
            send_sem=zc_send.at[stage, side],
            recv_sem=zc_recv.at[stage, side],
            device_id={"gx": gx, "gy": gy, "gz": gz + (2 * side - 1)},
            device_id_type=MESH,
        )

    def gathered(v, x, acc):
        return jnp.where(lane // 2 == x, pltpu.roll(v, 2 * x + 1, 1), acc)

    nothing = (jnp.zeros((tall, 128), f32),) * 3

    def send_columns(stage, first, acc):
        for c in range(3):
            swapped = jnp.where(even, pltpu.roll(acc[c], 127, 1), pltpu.roll(acc[c], 1, 1))
            zsend[stage, c, first : first + tall] = swapped
        for side in (0, 1):
            pl.when(has[side])(columns(stage, side).start)

    def take_columns(stage, first, scaled):
        for side in (0, 1):
            pl.when(has[1 - side])(columns(stage, side).wait_recv)
            pl.when(has[side])(columns(stage, side).wait_send)
        e = []
        for c in range(3):
            v = jnp.where(
                even, zgot[stage, 1, c, first - 1 : first - 1 + tall], zgot[stage, 0, c, first - 1 : first - 1 + tall]
            ) - zsend[stage, c, first - 1 : first - 1 + tall]
            edge[c, first - 1 : first - 1 + tall] = v

        def at(c, dy):
            return edge[c, first + dy : first + dy + tall]

        def along(v):
            return pltpu.roll(v, 126, 1) - pltpu.roll(v, 2, 1)

        ex_, ey_, ez_ = at(0, 0), at(1, 0), at(2, 0)
        fx = 0.25 * ex_ + sign * along(ez_)
        fy = 0.25 * ey_ + sign * (at(2, 1) - at(2, -1))
        fz = 0.875 * ez_ + sign * (along(ex_) + (at(1, 1) - at(1, -1)))
        for c, f in enumerate((fx, fy, fz)):
            fix[c, first : first + tall] = cpack[first : first + tall] * f if scaled else f

    def stencil(u, x, r):
        def at(c, dx, dy):
            return u[c, x + dx, r + dy : r + dy + 8]

        here = [at(c, 0, 0) for c in range(3)]
        xp, xm = [at(c, 1, 0) for c in range(3)], [at(c, -1, 0) for c in range(3)]
        yp, ym = [at(c, 0, 1) for c in range(3)], [at(c, 0, -1) for c in range(3)]

        def along_z(even_part, odd_part):
            return pltpu.roll(even_part + odd_part, 127, 1) + pltpu.roll(even_part - odd_part, 1, 1)

        zx = along_z(here[0], 0.625 * (xp[2] - xm[2]))
        zy = along_z(here[1], 0.625 * (yp[2] - ym[2]))
        zz = along_z(3.5 * here[2], 0.625 * ((xp[0] - xm[0]) + (yp[1] - ym[1])))
        mx = (at(1, 1, 1) - at(1, 1, -1)) - (at(1, -1, 1) - at(1, -1, -1))
        my = (at(0, 1, 1) - at(0, -1, 1)) - (at(0, 1, -1) - at(0, -1, -1))
        t = (
            (yp[0] + ym[0]) + 3.5 * (xp[0] + xm[0]) + 0.625 * mx + zx,
            (xp[1] + xm[1]) + 3.5 * (yp[1] + ym[1]) + 0.625 * my + zy,
            (xp[2] + xm[2]) + (yp[2] + ym[2]) + zz,
        )
        return here, t

    def sweep(src, dst, depth):
        first = W - depth
        rows = up8(cy + 2 * depth)

        def at(x, _):
            for r in range(first, first + rows, 8):
                here, t = stencil(src, x, r)
                q = cquarter[x, r : r + 8]
                for c in range(3):
                    if src is ua:
                        dst[c, x, r : r + 8] = 1.4 * here[c] + q * t[c]
                    else:
                        dst[c, x, r : r + 8] = 0.4 * here[c] + (ua[c, x, r : r + 8] + q * t[c])
            return 0

        planes(first, W + cx + depth, at, 0, 5)

    def mend(u, depth, extra):
        first = W - depth
        part = slice(first, first + tall)

        def at(x, acc):
            out = []
            for c in range(3):
                v = u[c, x, part] + jnp.where(rim, pltpu.roll(fix[c, part], 127 - 2 * x, 1), 0.0)
                if extra is not None:
                    v = v + extra[c, x, part]
                u[c, x, part] = v
                out.append(gathered(v, x, acc[c]))
            return tuple(out)

        return planes(first, W + cx + depth, at, nothing, 6)

    def push(slot, acc, gamma, energy):
        line = jnp.zeros((1, 128), f32)
        for k in range(vectors):
            total = jnp.sum(jnp.sum(acc[k], axis=0, keepdims=True), axis=1, keepdims=True)
            line = jnp.where(lane1 == base + k, total, line)
        if gamma is not None:
            line = jnp.where(lane1 == (base + vectors) % 128, gamma, line)
            line = jnp.where(lane1 == (base + vectors + 1) % 128, energy, line)
        gsend[slot, 0:1] = line
        gat[slot, pl.ds(me, 1)] = line
        for other in others:
            pltpu.make_async_remote_copy(
                src_ref=gsend.at[slot, 0],
                dst_ref=gat.at[slot, me],
                send_sem=g_send.at[slot],
                recv_sem=g_recv.at[slot],
                device_id=other,
                device_id_type=MESH,
            ).start()

    def collect(slot):
        rest = gat.at[slot, pl.ds(0, n - 1)]
        pltpu.make_async_copy(rest, rest, g_recv.at[slot]).wait()
        pltpu.make_async_copy(rest, rest, g_send.at[slot]).wait()
        lines, both = [], jnp.zeros((8, 128), f32)
        for t in range(n // 8):
            tile = gat[slot, 8 * t : 8 * t + 8]
            lines.append(jnp.sum(jnp.where(lane8 // vectors == row8, tile, 0.0), axis=0, keepdims=True))
            both = both + tile
        g_at = (row8 * vectors + vectors) % 128
        gamma = jnp.sum(jnp.where(lane8 == g_at, both, 0.0), axis=0, keepdims=True)
        energy = jnp.sum(jnp.where(lane8 == g_at + 1, both, 0.0), axis=0, keepdims=True)
        return lines, jnp.sum(gamma, axis=1, keepdims=True), jnp.sum(energy, axis=1, keepdims=True)

    def restrict(x, values, acc):
        acc = list(acc)
        for c in range(3):
            for k in range(vectors):
                prod = defl[k, c, x] * values[c]
                for t in range(0, cy, 8):
                    acc[k] = acc[k] + prod[t : t + 8]
        return acc

    clean = (jnp.zeros((8, 128), f32),) * vectors
    load_forces.wait()
    load_defl.wait()

    def first_share(x, acc):
        return tuple(restrict(x, [zext[0, c, W + x, W : W + cy] for c in range(3)], acc))

    acc = lax.fori_loop(0, cx, first_share, clean)
    load_mass.wait()

    pl.semaphore_wait(barrier, n - 1)
    push(0, acc, None, None)
    for j in range(1, nz):
        for copy in slab_copies(j):
            copy.start()
    send_halo(*halo_z(0))
    send_halo(*halo_m)

    load_slots.wait()
    for j in range(1, nz):
        for copy in slab_copies(j):
            copy.wait_recv()
            copy.wait_send()

    width = min(512, order)
    w_rows = lax.broadcasted_iota(jnp.int32, (BLOCK, width), 0)

    def slot_line(t):
        line = jnp.zeros((1, 128), jnp.int32)
        for r in range(8):
            line = jnp.where(lane1 // vectors == r, slots[8 * t + r] * vectors + lane1 % vectors, line)
        return line

    def one_hot(i, j):
        line = jnp.concatenate([slot_line(j * (width // 128) + t) for t in range(width // 128)], axis=1)
        return jnp.where(w_rows + i * BLOCK == line, 1.0, 0.0)

    if blocks <= 4:
        for i in range(blocks):
            right = one_hot(i, 0)
            if i:
                at = slice((i % per_slab) * BLOCK, (i % per_slab + 1) * BLOCK)
                right = right - dot(full[i // per_slab, at, 0 : i * BLOCK], sol_mat[0 : i * BLOCK])
            sol_mat[i * BLOCK : (i + 1) * BLOCK] = dot(inv[i], right)
    else:
        def wipe(i, _):
            sol_mat[pl.ds(pl.multiple_of(i * 8, 8), 8), :] = jnp.zeros((8, order), f32)
            return 0

        lax.fori_loop(0, order // 8, wipe, 0)

        def substitute(i, _):
            at = pl.ds(pl.multiple_of((i % per_slab) * BLOCK, BLOCK), BLOCK)
            for j in range(order // width):
                col = slice(j * width, (j + 1) * width)
                right = one_hot(i, j) - dot(full[i // per_slab, at, :], sol_mat[:, col])
                sol_mat[pl.ds(pl.multiple_of(i * BLOCK, BLOCK), BLOCK), col] = dot(inv[i], right)
            return 0

        lax.fori_loop(0, blocks, substitute, 0)

    mine = pl.ds(pl.multiple_of((me // 8) * 128, 128), 128)

    def turn(i, _):
        at = pl.ds(pl.multiple_of(i * BLOCK, BLOCK), BLOCK)
        turned[:, at] = sol_mat[at, mine].T
        return 0

    lax.fori_loop(0, blocks, turn, 0)
    own_rows = pl.ds(pl.multiple_of(base, 8), vectors)

    def form(j, _):
        col = pl.ds(pl.multiple_of(j * width, width), width)
        krows[:, col] = dot(turned[own_rows, :], sol_mat[:, col])
        return 0

    lax.fori_loop(0, order // width, form, 0)

    def coarse():
        y = jnp.zeros((vectors, 128), f32)
        for t in range(order // 128):
            y = y + krows[:, t * 128 : (t + 1) * 128] * gres[t]
        y = jnp.broadcast_to(jnp.sum(y, axis=1, keepdims=True), (vectors, 128))
        spread = [jnp.broadcast_to(y[k : k + 1], (8, 128)) for k in range(vectors)]

        def correct(x, _):
            for c in range(3):
                for t in range(0, cy, 8):
                    acc = spread[0] * defl[0, c, x, t : t + 8]
                    for k in range(1, vectors):
                        acc = acc + spread[k] * defl[k, c, x, t : t + 8]
                    cor[c, W + x, W + t : W + t + 8] = acc
            return 0

        lax.fori_loop(0, cx, correct, 0)

    lines, _, _ = collect(0)
    for t in range(n // 8):
        gres[t] = lines[t]
        gdir[t] = jnp.zeros((1, 128), f32)
    coarse()
    send_halo(*thin)
    take_halo(*halo_z(0))
    take_halo(*halo_m)
    rows = lax.broadcasted_iota(jnp.int32, (pitch, 128), 0)
    y_ok = ((rows >= W) | (gy > 0)) & ((rows < W + cy) | (gy < ny - 1)) & (rows < cy + 2 * W)

    def settle(x, acc):
        x_ok = ((x >= W) | (gx > 0)) & ((x < W + cx) | (gx < nx - 1))
        keep = jnp.where(x_ok, 1.0, 0.0)
        v = jnp.where(y_ok, 0.6 / (mext[0, x] + 2.75), 0.0) * keep
        cext[x] = v
        cquarter[x] = 0.25 * v
        out = [gathered(v[0:tall], x, acc[3])]
        new = []
        for c in range(3):
            f = zext[0, c, x]
            rext[c, x] = f
            idir[c, x] = jnp.zeros((pitch, 128), f32)
            u = v[0:tall] * f[0:tall]
            ua[c, x, 0:tall] = u
            new.append(gathered(u, x, acc[c]))
        return tuple(new) + tuple(out)

    acc = planes(0, ex, settle, nothing + (nothing[0],), 2)
    cpack[0:tall] = acc[3]
    send_columns(0, 0, acc[0:3])

    def own_clear(x, _):
        for c in range(3):
            sol[c, x] = jnp.zeros((cy, 128), f32)
            direc[c, x] = jnp.zeros((cy, 128), f32)
        return 0

    lax.fori_loop(0, cx, own_clear, 0)

    def iterate(it, carry):
        gamma_prior, step_prior = carry
        slot = (it + 1) % 2
        sweep(ua, ub, 2)
        take_columns(0, 1, True)
        acc = mend(ub, 2, None)
        send_columns(1, 1, acc)
        sweep(ub, uz, 1)
        take_columns(1, 2, True)
        take_halo(*thin)
        acc = mend(uz, 1, cor)
        send_columns(2, 2, acc)

        def image(x, _):
            for t in range(0, cy, 8):
                here, off = stencil(uz, x, W + t)
                diag = mext[0, x, W + t : W + t + 8] + 2.75
                for c in range(3):
                    zext[slot, c, x, W + t : W + t + 8] = diag * here[c] - 0.25 * off[c]
            return 0

        planes(W, W + cx, image, 0, 4)
        take_columns(2, 3, False)

        def finish(x, carry):
            gam, ene, acc = carry[0], carry[1], carry[2:]
            values = []
            for c in range(3):
                f = pltpu.roll(fix[c, W : W + cy], 127 - 2 * W - 2 * x, 1)
                a = zext[slot, c, W + x, W : W + cy] - jnp.where(rim_own, f, 0.0)
                zext[slot, c, W + x, W : W + cy] = a
                z = uz[c, W + x, W : W + cy]
                gam = gam + rext[c, W + x, W : W + cy] * z
                ene = ene + z * a
                values.append(a)
            return (gam, ene) + tuple(restrict(x, values, acc))

        blank = jnp.zeros((cy, 128), f32)
        carry = planes(0, cx, finish, (blank, blank) + clean, 2)
        gam = jnp.sum(jnp.sum(carry[0], axis=0, keepdims=True), axis=1, keepdims=True)
        ene = jnp.sum(jnp.sum(carry[1], axis=0, keepdims=True), axis=1, keepdims=True)
        push(slot, carry[2:], gam, ene)

        @pl.when(it < ITERS - 1)
        def _():
            send_halo(*halo_z(slot))

        lines, gamma, energy = collect(slot)
        momentum = jnp.where(it == 0, 0.0, gamma / gamma_prior)
        step = gamma / (energy - momentum * gamma / step_prior)

        @pl.when(it < ITERS - 1)
        def _():
            for t in range(n // 8):
                image_line = lines[t] + momentum * gdir[t]
                gdir[t] = image_line
                gres[t] = gres[t] - step * image_line
            coarse()
            send_halo(*thin)
            take_halo(*halo_z(slot))

            def update(x, acc):
                out = []
                for c in range(3):
                    image_dir = zext[slot, c, x, 0:tall] + momentum * idir[c, x, 0:tall]
                    idir[c, x, 0:tall] = image_dir
                    r = rext[c, x, 0:tall] - step * image_dir
                    rext[c, x, 0:tall] = r
                    u = cext[x, 0:tall] * r
                    ua[c, x, 0:tall] = u
                    out.append(gathered(u, x, acc[c]))
                return tuple(out)

            acc = planes(0, ex, update, nothing, 11)
            send_columns(0, 0, acc)

        def advance(x, _):
            for c in range(3):
                d = uz[c, W + x, W : W + cy] + momentum * direc[c, x]
                direc[c, x] = d
                sol[c, x] = sol[c, x] + step * d
            return 0

        lax.fori_loop(0, cx, advance, 0)

        @pl.when(it == ITERS - 1)
        def _():
            def give(x, _):
                for c in range(3):
                    image_dir = zext[slot, c, W + x, W : W + cy] + momentum * idir[c, W + x, W : W + cy]
                    res[c, x] = rext[c, W + x, W : W + cy] - step * image_dir
                return 0

            lax.fori_loop(0, cx, give, 0)

        return gamma, step

    one = jnp.ones((1, 1), f32)
    lax.fori_loop(0, ITERS, iterate, (one, one))


def solution(mesh):
    nx, ny, nz = mesh.shape["gx"], mesh.shape["gy"], mesh.shape["gz"]

    def body(forces, mass_shift, deflation, coarse_factor, coarse_slot):
        vectors = deflation.shape[0]
        cx, cy = forces.shape[1], forces.shape[2]
        order = coarse_factor.shape[1]
        slab = coarse_factor.shape[0]
        n = nx * ny * nz
        ex, pitch = cx + 2 * W, up8(up8(cy + 2 * W) + W)
        f32 = jnp.float32
        vm = lambda *shape: pltpu.VMEM(shape, f32)
        field = (3, ex, pitch, 128)
        dma = pltpu.SemaphoreType.DMA
        peers = max(nz - 1, 1)
        return pl.pallas_call(
            functools.partial(kernel, (nx, ny, nz, cx, cy, vectors, order)),
            out_shape=[jax.ShapeDtypeStruct(forces.shape, f32)] * 3,
            in_specs=[pl.BlockSpec(memory_space=pl.ANY)] * 5,
            out_specs=[pl.BlockSpec(memory_space=pltpu.VMEM)] * 3,
            scratch_shapes=[
                vm(2, *field), vm(*field), vm(*field), vm(ex, pitch, 128), vm(ex, pitch, 128),
                vm(1, ex, pitch, 128), vm(*field), vm(*field), vm(*field), vm(*field),
                vm(3, 3, pitch, 128), vm(3, 2, 3, pitch, 128), vm(3, pitch, 128), vm(3, pitch, 128),
                vm(pitch, 128), vm(*deflation.shape),
                vm(nz, slab, order), vm(order // BLOCK, BLOCK, BLOCK), vm(order, order),
                vm(BLOCK, order), vm(vectors, order),
                vm(2, 8, 128), vm(2, n, 128), vm(n // 8, 1, 128), vm(n // 8, 1, 128),
                pltpu.SMEM(coarse_slot.shape, jnp.int32),
                dma((8,)), dma((2, 8)), dma((8,)), dma((8,)), dma((8,)), dma((8,)),
                dma((3, 2)), dma((3, 2)), dma((2,)), dma((2,)),
                dma((peers,)), dma((peers,)), dma((peers,)), dma((peers,)), dma((5,)),
            ],
            compiler_params=pltpu.CompilerParams(
                collective_id=0, has_side_effects=True, vmem_limit_bytes=66 * 1000 * 1000
            ),
        )(forces, mass_shift, deflation, coarse_factor, coarse_slot)

    return jax.shard_map(
        body,
        mesh=mesh,
        in_specs=(
            P(None, "gx", "gy", "gz"),
            P("gx", "gy", "gz"),
            P(None, None, "gx", "gy", "gz"),
            P("gz", None),
            P(),
        ),
        out_specs=(P(None, "gx", "gy", "gz"), P(None, "gx", "gy", "gz"), P(None, "gx", "gy", "gz")),
        check_vma=False,
    )
```

```python
import functools

import jax
import jax.numpy as jnp
from jax import lax
from jax.experimental import pallas as pl
from jax.experimental.pallas import tpu as pltpu
from jax.sharding import PartitionSpec as P

SWEEPS = 3
ITERS = 4
MESH = pl.DeviceIdType.MESH
HIGHEST = lax.Precision.HIGHEST
W = SWEEPS
DIRS = ((0, -1), (0, 1), (-1, 0), (1, 0), (-1, -1), (-1, 1), (1, -1), (1, 1))
BLOCK = 128


def dot(a, b):
    return jnp.dot(a, b, precision=HIGHEST, preferred_element_type=jnp.float32)


def up8(v):
    return -(-v // 8) * 8


def planes(first, last, body, carry, most):
    count = last - first
    step = max(d for d in range(1, most + 1) if count % d == 0)

    def some(i, carry):
        for j in range(step):
            carry = body(first + i * step + j, carry)
        return carry

    return lax.fori_loop(0, count // step, some, carry)


def kernel(
    sizes,
    forces, mass, defl_hbm, factor, slots_hbm,
    out,
    zext, rext, idir, cext, cquarter, mext, cor, ua, ub, uz,
    zsend, zgot, edge, fix, cpack, defl,
    full, inv, sol_mat, turned, krows, gsend, gat, gres, gdir, slots,
    zx_send, zx_recv, c_send, c_recv, m_send, m_recv,
    zc_send, zc_recv, g_send, g_recv, f_send, f_recv, i_send, i_recv, local,
):
    nx, ny, nz, cx, cy, vectors, order = sizes
    n = nx * ny * nz
    sol, res, direc = out.at[0], out.at[1], out.at[2]
    ex = cx + 2 * W
    pitch = zext.shape[3]
    tall = up8(cy + 2 * W)
    gx, gy, gz = lax.axis_index("gx"), lax.axis_index("gy"), lax.axis_index("gz")
    me = (gx * ny + gy) * nz + gz
    f32 = jnp.float32

    def wrap(a, d, size):
        s = a + d
        return jnp.where(s >= size, s - size, s)

    others = [
        {"gx": wrap(gx, dx, nx), "gy": wrap(gy, dy, ny), "gz": wrap(gz, dz, nz)}
        for dx in range(nx) for dy in range(ny) for dz in range(nz) if (dx, dy, dz) != (0, 0, 0)
    ]
    own_x, own_y = pl.ds(W, cx), pl.ds(W, cy)
    load_factor = pltpu.make_async_copy(factor, full.at[gz], local.at[0])
    load_factor.start()
    load_slots = pltpu.make_async_copy(slots_hbm, slots, local.at[1])
    load_slots.start()

    def clear(ref):
        lead = ref.shape[0]
        zero = jnp.zeros(ref.shape[2:], f32)

        def one(i, _):
            for c in range(lead):
                ref[c, i] = zero
            return 0

        lax.fori_loop(0, ref.shape[1], one, 0)

    for ref in (zext.at[0], zext.at[1], mext, cor):
        clear(ref)
    zgot[...] = jnp.zeros(zgot.shape, f32)
    barrier = pltpu.get_barrier_semaphore()
    for other in others:
        pl.semaphore_signal(barrier, inc=1, device_id=other, device_id_type=MESH)
    load_forces = pltpu.make_async_copy(forces, zext.at[0, :, own_x, own_y], local.at[2])
    load_forces.start()
    load_mass = pltpu.make_async_copy(mass, mext.at[0, own_x, own_y], local.at[3])
    load_mass.start()
    load_defl = pltpu.make_async_copy(defl_hbm, defl, local.at[4])
    load_defl.start()
    for ref in (ua, ub, uz):
        clear(ref)
    for ref in (zsend, edge, fix, cpack):
        ref[...] = jnp.zeros(ref.shape, f32)

    lane = lax.broadcasted_iota(jnp.int32, (tall, 128), 1)
    lane8 = lax.broadcasted_iota(jnp.int32, (8, 128), 1)
    row8 = lax.broadcasted_iota(jnp.int32, (8, 128), 0)
    lane1 = lax.broadcasted_iota(jnp.int32, (1, 128), 1)
    rim = (lane == 0) | (lane == 127)
    rim_own = (lax.broadcasted_iota(jnp.int32, (cy, 128), 1) + 1) % 128 < 2
    even = lane % 2 == 0
    sign = jnp.where(even, 0.15625, -0.15625)
    base = (me % 8) * vectors

    slab = order // nz
    per_slab = slab // BLOCK
    blocks = order // BLOCK
    r_i = lax.broadcasted_iota(jnp.int32, (BLOCK, BLOCK), 0)
    c_i = lax.broadcasted_iota(jnp.int32, (BLOCK, BLOCK), 1)
    load_factor.wait()
    lows, xs = [], []
    for q in range(per_slab):
        col = pl.ds(pl.multiple_of((gz * per_slab + q) * BLOCK, BLOCK), BLOCK)
        block = full[gz, q * BLOCK : (q + 1) * BLOCK, col]
        lows.append(block)
        xs.append(jnp.where(r_i == c_i, 1.0 / jnp.where(r_i == c_i, block, 1.0), 0.0))
    s = 1
    while s < BLOCK:
        pick = (r_i // (2 * s) == c_i // (2 * s)) & ((r_i // s) % 2 == 1) & ((c_i // s) % 2 == 0)
        mids = [dot(jnp.where(pick, lows[q], 0.0), xs[q]) for q in range(per_slab)]
        xs = [xs[q] - dot(xs[q], mids[q]) for q in range(per_slab)]
        s *= 2
    for q in range(per_slab):
        inv[gz * per_slab + q] = xs[q]

    def slab_copies(j):
        t = wrap(gz, j, nz)
        to = {"gx": gx, "gy": gy, "gz": t}
        mine = pl.ds(gz * per_slab, per_slab)
        return (
            pltpu.make_async_remote_copy(
                src_ref=full.at[gz], dst_ref=full.at[gz], send_sem=f_send.at[j - 1],
                recv_sem=f_recv.at[j - 1], device_id=to, device_id_type=MESH,
            ),
            pltpu.make_async_remote_copy(
                src_ref=inv.at[mine], dst_ref=inv.at[mine], send_sem=i_send.at[j - 1],
                recv_sem=i_recv.at[j - 1], device_id=to, device_id_type=MESH,
            ),
        )

    def exists(dx, dy):
        ok = jnp.bool_(True)
        if dx < 0:
            ok = jnp.logical_and(ok, gx > 0)
        if dx > 0:
            ok = jnp.logical_and(ok, gx < nx - 1)
        if dy < 0:
            ok = jnp.logical_and(ok, gy > 0)
        if dy > 0:
            ok = jnp.logical_and(ok, gy < ny - 1)
        return ok

    def span(d, size, width):
        if d == 0:
            return pl.ds(W, size), pl.ds(W, size)
        if d < 0:
            return pl.ds(W, width), pl.ds(W + size, width)
        return pl.ds(W + size - width, width), pl.ds(W - width, width)

    def pieces(ext, width, send, recv):
        out = []
        for d, (dx, dy) in enumerate(DIRS):
            sx, tx = span(dx, cx, width)
            sy, ty = span(dy, cy, width)
            copy = pltpu.make_async_remote_copy(
                src_ref=ext.at[:, sx, sy],
                dst_ref=ext.at[:, tx, ty],
                send_sem=send.at[d],
                recv_sem=recv.at[d],
                device_id={"gx": gx + dx, "gy": gy + dy, "gz": gz},
                device_id_type=MESH,
            )
            out.append((dx, dy, copy))
        return out

    def send_halo(*args):
        for dx, dy, copy in pieces(*args):
            pl.when(exists(dx, dy))(copy.start)

    def take_halo(*args):
        for dx, dy, copy in pieces(*args):
            pl.when(exists(-dx, -dy))(copy.wait_recv)
            pl.when(exists(dx, dy))(copy.wait_send)

    def halo_z(slot):
        return zext.at[slot], W, zx_send, zx_recv.at[slot]

    halo_m = (mext, W, m_send, m_recv)
    thin = (cor, 1, c_send, c_recv)

    has = (gz > 0, gz < nz - 1)

    def columns(stage, side):
        return pltpu.make_async_remote_copy(
            src_ref=zsend.at[stage],
            dst_ref=zgot.at[stage, 1 - side],
            send_sem=zc_send.at[stage, side],
            recv_sem=zc_recv.at[stage, side],
            device_id={"gx": gx, "gy": gy, "gz": gz + (2 * side - 1)},
            device_id_type=MESH,
        )

    def gathered(v, x, acc):
        return jnp.where(lane // 2 == x, pltpu.roll(v, 2 * x + 1, 1), acc)

    nothing = (jnp.zeros((tall, 128), f32),) * 3

    def send_columns(stage, first, acc):
        for c in range(3):
            swapped = jnp.where(even, pltpu.roll(acc[c], 127, 1), pltpu.roll(acc[c], 1, 1))
            zsend[stage, c, first : first + tall] = swapped
        for side in (0, 1):
            pl.when(has[side])(columns(stage, side).start)

    def take_columns(stage, first, scaled):
        for side in (0, 1):
            pl.when(has[1 - side])(columns(stage, side).wait_recv)
            pl.when(has[side])(columns(stage, side).wait_send)
        e = []
        for c in range(3):
            v = jnp.where(
                even, zgot[stage, 1, c, first - 1 : first - 1 + tall], zgot[stage, 0, c, first - 1 : first - 1 + tall]
            ) - zsend[stage, c, first - 1 : first - 1 + tall]
            edge[c, first - 1 : first - 1 + tall] = v

        def at(c, dy):
            return edge[c, first + dy : first + dy + tall]

        def along(v):
            return pltpu.roll(v, 126, 1) - pltpu.roll(v, 2, 1)

        ex_, ey_, ez_ = at(0, 0), at(1, 0), at(2, 0)
        fx = 0.25 * ex_ + sign * along(ez_)
        fy = 0.25 * ey_ + sign * (at(2, 1) - at(2, -1))
        fz = 0.875 * ez_ + sign * (along(ex_) + (at(1, 1) - at(1, -1)))
        for c, f in enumerate((fx, fy, fz)):
            fix[c, first : first + tall] = cpack[first : first + tall] * f if scaled else f

    def stencil(u, x, r):
        def at(c, dx, dy):
            return u[c, x + dx, r + dy : r + dy + 8]

        here = [at(c, 0, 0) for c in range(3)]
        xp, xm = [at(c, 1, 0) for c in range(3)], [at(c, -1, 0) for c in range(3)]
        yp, ym = [at(c, 0, 1) for c in range(3)], [at(c, 0, -1) for c in range(3)]

        def along_z(even_part, odd_part):
            return pltpu.roll(even_part + odd_part, 127, 1) + pltpu.roll(even_part - odd_part, 1, 1)

        zx = along_z(here[0], 0.625 * (xp[2] - xm[2]))
        zy = along_z(here[1], 0.625 * (yp[2] - ym[2]))
        zz = along_z(3.5 * here[2], 0.625 * ((xp[0] - xm[0]) + (yp[1] - ym[1])))
        mx = (at(1, 1, 1) - at(1, 1, -1)) - (at(1, -1, 1) - at(1, -1, -1))
        my = (at(0, 1, 1) - at(0, -1, 1)) - (at(0, 1, -1) - at(0, -1, -1))
        t = (
            (yp[0] + ym[0]) + 3.5 * (xp[0] + xm[0]) + 0.625 * mx + zx,
            (xp[1] + xm[1]) + 3.5 * (yp[1] + ym[1]) + 0.625 * my + zy,
            (xp[2] + xm[2]) + (yp[2] + ym[2]) + zz,
        )
        return here, t

    def sweep(src, dst, depth):
        first = W - depth
        rows = up8(cy + 2 * depth)

        def at(x, _):
            for r in range(first, first + rows, 8):
                here, t = stencil(src, x, r)
                q = cquarter[x, r : r + 8]
                for c in range(3):
                    if src is ua:
                        dst[c, x, r : r + 8] = 1.4 * here[c] + q * t[c]
                    else:
                        dst[c, x, r : r + 8] = 0.4 * here[c] + (ua[c, x, r : r + 8] + q * t[c])
            return 0

        planes(first, W + cx + depth, at, 0, 5)

    def mend(u, depth, extra):
        first = W - depth
        part = slice(first, first + tall)

        def at(x, acc):
            out = []
            for c in range(3):
                v = u[c, x, part] + jnp.where(rim, pltpu.roll(fix[c, part], 127 - 2 * x, 1), 0.0)
                if extra is not None:
                    v = v + extra[c, x, part]
                u[c, x, part] = v
                out.append(gathered(v, x, acc[c]))
            return tuple(out)

        return planes(first, W + cx + depth, at, nothing, 6)

    def push(slot, acc, gamma, energy):
        line = jnp.zeros((1, 128), f32)
        for k in range(vectors):
            total = jnp.sum(jnp.sum(acc[k], axis=0, keepdims=True), axis=1, keepdims=True)
            line = jnp.where(lane1 == base + k, total, line)
        if gamma is not None:
            line = jnp.where(lane1 == (base + vectors) % 128, gamma, line)
            line = jnp.where(lane1 == (base + vectors + 1) % 128, energy, line)
        gsend[slot, 0:1] = line
        gat[slot, pl.ds(me, 1)] = line
        for other in others:
            pltpu.make_async_remote_copy(
                src_ref=gsend.at[slot, 0],
                dst_ref=gat.at[slot, me],
                send_sem=g_send.at[slot],
                recv_sem=g_recv.at[slot],
                device_id=other,
                device_id_type=MESH,
            ).start()

    def collect(slot):
        rest = gat.at[slot, pl.ds(0, n - 1)]
        pltpu.make_async_copy(rest, rest, g_recv.at[slot]).wait()
        pltpu.make_async_copy(rest, rest, g_send.at[slot]).wait()
        lines, both = [], jnp.zeros((8, 128), f32)
        for t in range(n // 8):
            tile = gat[slot, 8 * t : 8 * t + 8]
            lines.append(jnp.sum(jnp.where(lane8 // vectors == row8, tile, 0.0), axis=0, keepdims=True))
            both = both + tile
        g_at = (row8 * vectors + vectors) % 128
        gamma = jnp.sum(jnp.where(lane8 == g_at, both, 0.0), axis=0, keepdims=True)
        energy = jnp.sum(jnp.where(lane8 == g_at + 1, both, 0.0), axis=0, keepdims=True)
        return lines, jnp.sum(gamma, axis=1, keepdims=True), jnp.sum(energy, axis=1, keepdims=True)

    def restrict(x, values, acc):
        acc = list(acc)
        for c in range(3):
            for k in range(vectors):
                prod = defl[k, c, x] * values[c]
                for t in range(0, cy, 8):
                    acc[k] = acc[k] + prod[t : t + 8]
        return acc

    clean = (jnp.zeros((8, 128), f32),) * vectors
    load_forces.wait()
    load_defl.wait()

    def first_share(x, acc):
        return tuple(restrict(x, [zext[0, c, W + x, W : W + cy] for c in range(3)], acc))

    acc = lax.fori_loop(0, cx, first_share, clean)
    load_mass.wait()

    pl.semaphore_wait(barrier, n - 1)
    push(0, acc, None, None)
    for j in range(1, nz):
        for copy in slab_copies(j):
            copy.start()
    send_halo(*halo_z(0))
    send_halo(*halo_m)

    load_slots.wait()
    for j in range(1, nz):
        for copy in slab_copies(j):
            copy.wait_recv()
            copy.wait_send()

    width = min(512, order)
    w_rows = lax.broadcasted_iota(jnp.int32, (BLOCK, width), 0)

    def slot_line(t):
        line = jnp.zeros((1, 128), jnp.int32)
        for r in range(8):
            line = jnp.where(lane1 // vectors == r, slots[8 * t + r] * vectors + lane1 % vectors, line)
        return line

    def one_hot(i, j):
        line = jnp.concatenate([slot_line(j * (width // 128) + t) for t in range(width // 128)], axis=1)
        return jnp.where(w_rows + i * BLOCK == line, 1.0, 0.0)

    if blocks <= 4:
        for i in range(blocks):
            right = one_hot(i, 0)
            if i:
                at = slice((i % per_slab) * BLOCK, (i % per_slab + 1) * BLOCK)
                right = right - dot(full[i // per_slab, at, 0 : i * BLOCK], sol_mat[0 : i * BLOCK])
            sol_mat[i * BLOCK : (i + 1) * BLOCK] = dot(inv[i], right)
    else:
        def wipe(i, _):
            sol_mat[pl.ds(pl.multiple_of(i * 8, 8), 8), :] = jnp.zeros((8, order), f32)
            return 0

        lax.fori_loop(0, order // 8, wipe, 0)

        def substitute(i, _):
            at = pl.ds(pl.multiple_of((i % per_slab) * BLOCK, BLOCK), BLOCK)
            for j in range(order // width):
                col = slice(j * width, (j + 1) * width)
                right = one_hot(i, j) - dot(full[i // per_slab, at, :], sol_mat[:, col])
                sol_mat[pl.ds(pl.multiple_of(i * BLOCK, BLOCK), BLOCK), col] = dot(inv[i], right)
            return 0

        lax.fori_loop(0, blocks, substitute, 0)

    mine = pl.ds(pl.multiple_of((me // 8) * 128, 128), 128)

    def turn(i, _):
        at = pl.ds(pl.multiple_of(i * BLOCK, BLOCK), BLOCK)
        turned[:, at] = sol_mat[at, mine].T
        return 0

    lax.fori_loop(0, blocks, turn, 0)
    own_rows = pl.ds(pl.multiple_of(base, 8), vectors)

    def form(j, _):
        col = pl.ds(pl.multiple_of(j * width, width), width)
        krows[:, col] = dot(turned[own_rows, :], sol_mat[:, col])
        return 0

    lax.fori_loop(0, order // width, form, 0)

    def coarse():
        y = jnp.zeros((vectors, 128), f32)
        for t in range(order // 128):
            y = y + krows[:, t * 128 : (t + 1) * 128] * gres[t]
        y = jnp.broadcast_to(jnp.sum(y, axis=1, keepdims=True), (vectors, 128))
        spread = [jnp.broadcast_to(y[k : k + 1], (8, 128)) for k in range(vectors)]

        def correct(x, _):
            for c in range(3):
                for t in range(0, cy, 8):
                    acc = spread[0] * defl[0, c, x, t : t + 8]
                    for k in range(1, vectors):
                        acc = acc + spread[k] * defl[k, c, x, t : t + 8]
                    cor[c, W + x, W + t : W + t + 8] = acc
            return 0

        lax.fori_loop(0, cx, correct, 0)

    lines, _, _ = collect(0)
    for t in range(n // 8):
        gres[t] = lines[t]
        gdir[t] = jnp.zeros((1, 128), f32)
    coarse()
    send_halo(*thin)
    take_halo(*halo_z(0))
    take_halo(*halo_m)
    rows = lax.broadcasted_iota(jnp.int32, (pitch, 128), 0)
    y_ok = ((rows >= W) | (gy > 0)) & ((rows < W + cy) | (gy < ny - 1)) & (rows < cy + 2 * W)

    def settle(x, acc):
        x_ok = ((x >= W) | (gx > 0)) & ((x < W + cx) | (gx < nx - 1))
        keep = jnp.where(x_ok, 1.0, 0.0)
        v = jnp.where(y_ok, 0.6 / (mext[0, x] + 2.75), 0.0) * keep
        cext[x] = v
        cquarter[x] = 0.25 * v
        out = [gathered(v[0:tall], x, acc[3])]
        new = []
        for c in range(3):
            f = zext[0, c, x]
            rext[c, x] = f
            idir[c, x] = jnp.zeros((pitch, 128), f32)
            u = v[0:tall] * f[0:tall]
            ua[c, x, 0:tall] = u
            new.append(gathered(u, x, acc[c]))
        return tuple(new) + tuple(out)

    acc = planes(0, ex, settle, nothing + (nothing[0],), 2)
    cpack[0:tall] = acc[3]
    send_columns(0, 0, acc[0:3])

    def own_clear(x, _):
        for c in range(3):
            sol[c, x] = jnp.zeros((cy, 128), f32)
            direc[c, x] = jnp.zeros((cy, 128), f32)
        return 0

    lax.fori_loop(0, cx, own_clear, 0)

    def iterate(it, carry):
        gamma_prior, step_prior = carry
        slot = (it + 1) % 2
        sweep(ua, ub, 2)
        take_columns(0, 1, True)
        acc = mend(ub, 2, None)
        send_columns(1, 1, acc)
        sweep(ub, uz, 1)
        take_columns(1, 2, True)
        take_halo(*thin)
        acc = mend(uz, 1, cor)
        send_columns(2, 2, acc)

        def image(x, _):
            for t in range(0, cy, 8):
                here, off = stencil(uz, x, W + t)
                diag = mext[0, x, W + t : W + t + 8] + 2.75
                for c in range(3):
                    zext[slot, c, x, W + t : W + t + 8] = diag * here[c] - 0.25 * off[c]
            return 0

        planes(W, W + cx, image, 0, 4)
        take_columns(2, 3, False)

        def finish(x, carry):
            gam, ene, acc = carry[0], carry[1], carry[2:]
            values = []
            for c in range(3):
                f = pltpu.roll(fix[c, W : W + cy], 127 - 2 * W - 2 * x, 1)
                a = zext[slot, c, W + x, W : W + cy] - jnp.where(rim_own, f, 0.0)
                zext[slot, c, W + x, W : W + cy] = a
                z = uz[c, W + x, W : W + cy]
                gam = gam + rext[c, W + x, W : W + cy] * z
                ene = ene + z * a
                values.append(a)
            return (gam, ene) + tuple(restrict(x, values, acc))

        blank = jnp.zeros((cy, 128), f32)
        carry = planes(0, cx, finish, (blank, blank) + clean, 2)
        gam = jnp.sum(jnp.sum(carry[0], axis=0, keepdims=True), axis=1, keepdims=True)
        ene = jnp.sum(jnp.sum(carry[1], axis=0, keepdims=True), axis=1, keepdims=True)
        push(slot, carry[2:], gam, ene)

        @pl.when(it < ITERS - 1)
        def _():
            send_halo(*halo_z(slot))

        lines, gamma, energy = collect(slot)
        momentum = jnp.where(it == 0, 0.0, gamma / gamma_prior)
        step = gamma / (energy - momentum * gamma / step_prior)

        @pl.when(it < ITERS - 1)
        def _():
            for t in range(n // 8):
                image_line = lines[t] + momentum * gdir[t]
                gdir[t] = image_line
                gres[t] = gres[t] - step * image_line
            coarse()
            send_halo(*thin)
            take_halo(*halo_z(slot))

            def update(x, acc):
                out = []
                for c in range(3):
                    image_dir = zext[slot, c, x, 0:tall] + momentum * idir[c, x, 0:tall]
                    idir[c, x, 0:tall] = image_dir
                    r = rext[c, x, 0:tall] - step * image_dir
                    rext[c, x, 0:tall] = r
                    u = cext[x, 0:tall] * r
                    ua[c, x, 0:tall] = u
                    out.append(gathered(u, x, acc[c]))
                return tuple(out)

            acc = planes(0, ex, update, nothing, 11)
            send_columns(0, 0, acc)

        def advance(x, _):
            for c in range(3):
                d = uz[c, W + x, W : W + cy] + momentum * direc[c, x]
                direc[c, x] = d
                sol[c, x] = sol[c, x] + step * d
            return 0

        lax.fori_loop(0, cx, advance, 0)

        @pl.when(it == ITERS - 1)
        def _():
            def give(x, _):
                for c in range(3):
                    image_dir = zext[slot, c, W + x, W : W + cy] + momentum * idir[c, W + x, W : W + cy]
                    res[c, x] = rext[c, W + x, W : W + cy] - step * image_dir
                return 0

            lax.fori_loop(0, cx, give, 0)

        return gamma, step

    one = jnp.ones((1, 1), f32)
    lax.fori_loop(0, ITERS, iterate, (one, one))


def hand_out(whole, *refs):
    outs, sems = refs[:-1], refs[-1]
    copies = [pltpu.make_async_copy(whole.at[i], out, sems.at[i]) for i, out in enumerate(outs)]
    for copy in copies:
        copy.start()
    for copy in copies:
        copy.wait()


def solution(mesh):
    nx, ny, nz = mesh.shape["gx"], mesh.shape["gy"], mesh.shape["gz"]

    def body(forces, mass_shift, deflation, coarse_factor, coarse_slot):
        vectors = deflation.shape[0]
        cx, cy = forces.shape[1], forces.shape[2]
        order = coarse_factor.shape[1]
        slab = coarse_factor.shape[0]
        n = nx * ny * nz
        ex, pitch = cx + 2 * W, up8(up8(cy + 2 * W) + W)
        f32 = jnp.float32
        vm = lambda *shape: pltpu.VMEM(shape, f32)
        field = (3, ex, pitch, 128)
        dma = pltpu.SemaphoreType.DMA
        peers = max(nz - 1, 1)
        room = 66 * 1000 * 1000
        whole = pl.pallas_call(
            functools.partial(kernel, (nx, ny, nz, cx, cy, vectors, order)),
            out_shape=jax.ShapeDtypeStruct((3, *forces.shape), f32),
            in_specs=[pl.BlockSpec(memory_space=pl.ANY)] * 5,
            out_specs=pl.BlockSpec(memory_space=pltpu.VMEM),
            scratch_shapes=[
                vm(2, *field), vm(*field), vm(*field), vm(ex, pitch, 128), vm(ex, pitch, 128),
                vm(1, ex, pitch, 128), vm(*field), vm(*field), vm(*field), vm(*field),
                vm(3, 3, pitch, 128), vm(3, 2, 3, pitch, 128), vm(3, pitch, 128), vm(3, pitch, 128),
                vm(pitch, 128), vm(*deflation.shape),
                vm(nz, slab, order), vm(order // BLOCK, BLOCK, BLOCK), vm(order, order),
                vm(BLOCK, order), vm(vectors, order),
                vm(2, 8, 128), vm(2, n, 128), vm(n // 8, 1, 128), vm(n // 8, 1, 128),
                pltpu.SMEM(coarse_slot.shape, jnp.int32),
                dma((8,)), dma((2, 8)), dma((8,)), dma((8,)), dma((8,)), dma((8,)),
                dma((3, 2)), dma((3, 2)), dma((2,)), dma((2,)),
                dma((peers,)), dma((peers,)), dma((peers,)), dma((peers,)), dma((5,)),
            ],
            compiler_params=pltpu.CompilerParams(
                collective_id=0, has_side_effects=True, vmem_limit_bytes=room
            ),
        )(forces, mass_shift, deflation, coarse_factor, coarse_slot)
        return pl.pallas_call(
            hand_out,
            out_shape=[jax.ShapeDtypeStruct(forces.shape, f32)] * 3,
            in_specs=[pl.BlockSpec(memory_space=pltpu.VMEM)],
            out_specs=[pl.BlockSpec(memory_space=pl.ANY)] * 3,
            scratch_shapes=[dma((3,))],
            compiler_params=pltpu.CompilerParams(vmem_limit_bytes=4 * 1000 * 1000),
        )(whole)

    return jax.shard_map(
        body,
        mesh=mesh,
        in_specs=(
            P(None, "gx", "gy", "gz"),
            P("gx", "gy", "gz"),
            P(None, None, "gx", "gy", "gz"),
            P("gz", None),
            P(),
        ),
        out_specs=(P(None, "gx", "gy", "gz"), P(None, "gx", "gy", "gz"), P(None, "gx", "gy", "gz")),
        check_vma=False,
    )
```

```python
import functools

import jax
import jax.numpy as jnp
from jax import lax
from jax.experimental import pallas as pl
from jax.experimental.pallas import tpu as pltpu
from jax.sharding import PartitionSpec as P

SWEEPS = 3
ITERS = 4
MESH = pl.DeviceIdType.MESH
HIGHEST = lax.Precision.HIGHEST
W = SWEEPS
DIRS = ((0, -1), (0, 1), (-1, 0), (1, 0), (-1, -1), (-1, 1), (1, -1), (1, 1))
BLOCK = 128


def dot(a, b):
    return jnp.dot(a, b, precision=HIGHEST, preferred_element_type=jnp.float32)


def up8(v):
    return -(-v // 8) * 8


def planes(first, last, body, carry, most):
    count = last - first
    step = max(d for d in range(1, most + 1) if count % d == 0)

    def some(i, carry):
        for j in range(step):
            carry = body(first + i * step + j, carry)
        return carry

    return lax.fori_loop(0, count // step, some, carry)


def kernel(
    sizes,
    forces, mass, defl_hbm, factor, slots_hbm,
    out,
    zext, rext, idir, cext, cquarter, mext, cor, ua, ub, uz,
    zsend, zgot, edge, fix, cpack, defl,
    full, inv, sol_mat, turned, krows, gsend, gat, gres, gdir, slots,
    zx_send, zx_recv, c_send, c_recv, m_send, m_recv,
    zc_send, zc_recv, g_send, g_recv, f_send, f_recv, i_send, i_recv, local,
):
    nx, ny, nz, cx, cy, vectors, order = sizes
    n = nx * ny * nz
    sol, res, direc = out.at[0], out.at[1], out.at[2]
    ex = cx + 2 * W
    pitch = zext.shape[3]
    tall = up8(cy + 2 * W)
    gx, gy, gz = lax.axis_index("gx"), lax.axis_index("gy"), lax.axis_index("gz")
    me = (gx * ny + gy) * nz + gz
    f32 = jnp.float32

    def wrap(a, d, size):
        s = a + d
        return jnp.where(s >= size, s - size, s)

    others = [
        {"gx": wrap(gx, dx, nx), "gy": wrap(gy, dy, ny), "gz": wrap(gz, dz, nz)}
        for dx in range(nx) for dy in range(ny) for dz in range(nz) if (dx, dy, dz) != (0, 0, 0)
    ]
    own_x, own_y = pl.ds(W, cx), pl.ds(W, cy)
    load_factor = pltpu.make_async_copy(factor, full.at[gz], local.at[0])
    load_factor.start()
    load_slots = pltpu.make_async_copy(slots_hbm, slots, local.at[1])
    load_slots.start()

    def clear(ref):
        lead = ref.shape[0]
        zero = jnp.zeros(ref.shape[2:], f32)

        def one(i, _):
            for c in range(lead):
                ref[c, i] = zero
            return 0

        lax.fori_loop(0, ref.shape[1], one, 0)

    for ref in (zext.at[0], zext.at[1], mext, cor):
        clear(ref)
    zgot[...] = jnp.zeros(zgot.shape, f32)
    barrier = pltpu.get_barrier_semaphore()
    for other in others:
        pl.semaphore_signal(barrier, inc=1, device_id=other, device_id_type=MESH)
    load_forces = pltpu.make_async_copy(forces, zext.at[0, :, own_x, own_y], local.at[2])
    load_forces.start()
    load_mass = pltpu.make_async_copy(mass, mext.at[0, own_x, own_y], local.at[3])
    load_mass.start()
    load_defl = pltpu.make_async_copy(defl_hbm, defl, local.at[4])
    load_defl.start()
    for ref in (ua, ub, uz):
        clear(ref)
    for ref in (zsend, edge, fix, cpack):
        ref[...] = jnp.zeros(ref.shape, f32)

    lane = lax.broadcasted_iota(jnp.int32, (tall, 128), 1)
    lane8 = lax.broadcasted_iota(jnp.int32, (8, 128), 1)
    row8 = lax.broadcasted_iota(jnp.int32, (8, 128), 0)
    lane1 = lax.broadcasted_iota(jnp.int32, (1, 128), 1)
    rim = (lane == 0) | (lane == 127)
    rim_own = (lax.broadcasted_iota(jnp.int32, (cy, 128), 1) + 1) % 128 < 2
    even = lane % 2 == 0
    sign = jnp.where(even, 0.15625, -0.15625)
    base = (me % 8) * vectors

    slab = order // nz
    per_slab = slab // BLOCK
    blocks = order // BLOCK
    r_i = lax.broadcasted_iota(jnp.int32, (BLOCK, BLOCK), 0)
    c_i = lax.broadcasted_iota(jnp.int32, (BLOCK, BLOCK), 1)
    load_factor.wait()
    lows, xs = [], []
    for q in range(per_slab):
        col = pl.ds(pl.multiple_of((gz * per_slab + q) * BLOCK, BLOCK), BLOCK)
        block = full[gz, q * BLOCK : (q + 1) * BLOCK, col]
        lows.append(block)
        xs.append(jnp.where(r_i == c_i, 1.0 / jnp.where(r_i == c_i, block, 1.0), 0.0))
    s = 1
    while s < BLOCK:
        pick = (r_i // (2 * s) == c_i // (2 * s)) & ((r_i // s) % 2 == 1) & ((c_i // s) % 2 == 0)
        mids = [dot(jnp.where(pick, lows[q], 0.0), xs[q]) for q in range(per_slab)]
        xs = [xs[q] - dot(xs[q], mids[q]) for q in range(per_slab)]
        s *= 2
    for q in range(per_slab):
        inv[gz * per_slab + q] = xs[q]

    def slab_copies(j):
        t = wrap(gz, j, nz)
        to = {"gx": gx, "gy": gy, "gz": t}
        mine = pl.ds(gz * per_slab, per_slab)
        return (
            pltpu.make_async_remote_copy(
                src_ref=full.at[gz], dst_ref=full.at[gz], send_sem=f_send.at[j - 1],
                recv_sem=f_recv.at[j - 1], device_id=to, device_id_type=MESH,
            ),
            pltpu.make_async_remote_copy(
                src_ref=inv.at[mine], dst_ref=inv.at[mine], send_sem=i_send.at[j - 1],
                recv_sem=i_recv.at[j - 1], device_id=to, device_id_type=MESH,
            ),
        )

    def exists(dx, dy):
        ok = jnp.bool_(True)
        if dx < 0:
            ok = jnp.logical_and(ok, gx > 0)
        if dx > 0:
            ok = jnp.logical_and(ok, gx < nx - 1)
        if dy < 0:
            ok = jnp.logical_and(ok, gy > 0)
        if dy > 0:
            ok = jnp.logical_and(ok, gy < ny - 1)
        return ok

    def span(d, size, width):
        if d == 0:
            return pl.ds(W, size), pl.ds(W, size)
        if d < 0:
            return pl.ds(W, width), pl.ds(W + size, width)
        return pl.ds(W + size - width, width), pl.ds(W - width, width)

    def pieces(ext, width, send, recv):
        out = []
        for d, (dx, dy) in enumerate(DIRS):
            sx, tx = span(dx, cx, width)
            sy, ty = span(dy, cy, width)
            copy = pltpu.make_async_remote_copy(
                src_ref=ext.at[:, sx, sy],
                dst_ref=ext.at[:, tx, ty],
                send_sem=send.at[d],
                recv_sem=recv.at[d],
                device_id={"gx": gx + dx, "gy": gy + dy, "gz": gz},
                device_id_type=MESH,
            )
            out.append((dx, dy, copy))
        return out

    def send_halo(*args):
        for dx, dy, copy in pieces(*args):
            pl.when(exists(dx, dy))(copy.start)

    def take_halo(*args):
        for dx, dy, copy in pieces(*args):
            pl.when(exists(-dx, -dy))(copy.wait_recv)
            pl.when(exists(dx, dy))(copy.wait_send)

    def halo_z(slot):
        return zext.at[slot], W, zx_send, zx_recv.at[slot]

    halo_m = (mext, W, m_send, m_recv)
    thin = (cor, 1, c_send, c_recv)

    has = (gz > 0, gz < nz - 1)

    def columns(stage, side):
        return pltpu.make_async_remote_copy(
            src_ref=zsend.at[stage],
            dst_ref=zgot.at[stage, 1 - side],
            send_sem=zc_send.at[stage, side],
            recv_sem=zc_recv.at[stage, side],
            device_id={"gx": gx, "gy": gy, "gz": gz + (2 * side - 1)},
            device_id_type=MESH,
        )

    def gathered(v, x, acc):
        return jnp.where(lane // 2 == x, pltpu.roll(v, 2 * x + 1, 1), acc)

    nothing = (jnp.zeros((tall, 128), f32),) * 3

    def send_columns(stage, first, acc):
        for c in range(3):
            swapped = jnp.where(even, pltpu.roll(acc[c], 127, 1), pltpu.roll(acc[c], 1, 1))
            zsend[stage, c, first : first + tall] = swapped
        for side in (0, 1):
            pl.when(has[side])(columns(stage, side).start)

    def take_columns(stage, first, scaled):
        for side in (0, 1):
            pl.when(has[1 - side])(columns(stage, side).wait_recv)
            pl.when(has[side])(columns(stage, side).wait_send)
        e = []
        for c in range(3):
            v = jnp.where(
                even, zgot[stage, 1, c, first - 1 : first - 1 + tall], zgot[stage, 0, c, first - 1 : first - 1 + tall]
            ) - zsend[stage, c, first - 1 : first - 1 + tall]
            edge[c, first - 1 : first - 1 + tall] = v

        def at(c, dy):
            return edge[c, first + dy : first + dy + tall]

        def along(v):
            return pltpu.roll(v, 126, 1) - pltpu.roll(v, 2, 1)

        ex_, ey_, ez_ = at(0, 0), at(1, 0), at(2, 0)
        fx = 0.25 * ex_ + sign * along(ez_)
        fy = 0.25 * ey_ + sign * (at(2, 1) - at(2, -1))
        fz = 0.875 * ez_ + sign * (along(ex_) + (at(1, 1) - at(1, -1)))
        for c, f in enumerate((fx, fy, fz)):
            fix[c, first : first + tall] = cpack[first : first + tall] * f if scaled else f

    def stencil(u, x, r):
        def at(c, dx, dy):
            return u[c, x + dx, r + dy : r + dy + 8]

        here = [at(c, 0, 0) for c in range(3)]
        xp, xm = [at(c, 1, 0) for c in range(3)], [at(c, -1, 0) for c in range(3)]
        yp, ym = [at(c, 0, 1) for c in range(3)], [at(c, 0, -1) for c in range(3)]

        def along_z(even_part, odd_part):
            return pltpu.roll(even_part + odd_part, 127, 1) + pltpu.roll(even_part - odd_part, 1, 1)

        zx = along_z(here[0], 0.625 * (xp[2] - xm[2]))
        zy = along_z(here[1], 0.625 * (yp[2] - ym[2]))
        zz = along_z(3.5 * here[2], 0.625 * ((xp[0] - xm[0]) + (yp[1] - ym[1])))
        mx = (at(1, 1, 1) - at(1, 1, -1)) - (at(1, -1, 1) - at(1, -1, -1))
        my = (at(0, 1, 1) - at(0, -1, 1)) - (at(0, 1, -1) - at(0, -1, -1))
        t = (
            (yp[0] + ym[0]) + 3.5 * (xp[0] + xm[0]) + 0.625 * mx + zx,
            (xp[1] + xm[1]) + 3.5 * (yp[1] + ym[1]) + 0.625 * my + zy,
            (xp[2] + xm[2]) + (yp[2] + ym[2]) + zz,
        )
        return here, t

    def sweep(src, dst, depth):
        first = W - depth
        rows = up8(cy + 2 * depth)

        def at(x, _):
            for r in range(first, first + rows, 8):
                here, t = stencil(src, x, r)
                q = cquarter[x, r : r + 8]
                for c in range(3):
                    if src is ua:
                        dst[c, x, r : r + 8] = 1.4 * here[c] + q * t[c]
                    else:
                        dst[c, x, r : r + 8] = 0.4 * here[c] + (ua[c, x, r : r + 8] + q * t[c])
            return 0

        planes(first, W + cx + depth, at, 0, 5)

    def mend(u, depth, extra):
        first = W - depth
        part = slice(first, first + tall)

        def at(x, acc):
            out = []
            for c in range(3):
                v = u[c, x, part] + jnp.where(rim, pltpu.roll(fix[c, part], 127 - 2 * x, 1), 0.0)
                if extra is not None:
                    v = v + extra[c, x, part]
                u[c, x, part] = v
                out.append(gathered(v, x, acc[c]))
            return tuple(out)

        return planes(first, W + cx + depth, at, nothing, 6)

    def push(slot, acc, gamma, energy):
        line = jnp.zeros((1, 128), f32)
        for k in range(vectors):
            total = jnp.sum(jnp.sum(acc[k], axis=0, keepdims=True), axis=1, keepdims=True)
            line = jnp.where(lane1 == base + k, total, line)
        if gamma is not None:
            line = jnp.where(lane1 == (base + vectors) % 128, gamma, line)
            line = jnp.where(lane1 == (base + vectors + 1) % 128, energy, line)
        gsend[slot, 0:1] = line
        gat[slot, pl.ds(me, 1)] = line
        for other in others:
            pltpu.make_async_remote_copy(
                src_ref=gsend.at[slot, 0],
                dst_ref=gat.at[slot, me],
                send_sem=g_send.at[slot],
                recv_sem=g_recv.at[slot],
                device_id=other,
                device_id_type=MESH,
            ).start()

    def collect(slot):
        rest = gat.at[slot, pl.ds(0, n - 1)]
        pltpu.make_async_copy(rest, rest, g_recv.at[slot]).wait()
        pltpu.make_async_copy(rest, rest, g_send.at[slot]).wait()
        lines, both = [], jnp.zeros((8, 128), f32)
        for t in range(n // 8):
            tile = gat[slot, 8 * t : 8 * t + 8]
            lines.append(jnp.sum(jnp.where(lane8 // vectors == row8, tile, 0.0), axis=0, keepdims=True))
            both = both + tile
        g_at = (row8 * vectors + vectors) % 128
        gamma = jnp.sum(jnp.where(lane8 == g_at, both, 0.0), axis=0, keepdims=True)
        energy = jnp.sum(jnp.where(lane8 == g_at + 1, both, 0.0), axis=0, keepdims=True)
        return lines, jnp.sum(gamma, axis=1, keepdims=True), jnp.sum(energy, axis=1, keepdims=True)

    def restrict(x, values, acc):
        acc = list(acc)
        for c in range(3):
            for k in range(vectors):
                prod = defl[k, c, x] * values[c]
                for t in range(0, cy, 8):
                    acc[k] = acc[k] + prod[t : t + 8]
        return acc

    clean = (jnp.zeros((8, 128), f32),) * vectors
    load_forces.wait()
    load_defl.wait()

    def first_share(x, acc):
        return tuple(restrict(x, [zext[0, c, W + x, W : W + cy] for c in range(3)], acc))

    acc = lax.fori_loop(0, cx, first_share, clean)
    load_mass.wait()

    pl.semaphore_wait(barrier, n - 1)
    push(0, acc, None, None)
    for j in range(1, nz):
        for copy in slab_copies(j):
            copy.start()
    send_halo(*halo_z(0))
    send_halo(*halo_m)

    load_slots.wait()
    for j in range(1, nz):
        for copy in slab_copies(j):
            copy.wait_recv()
            copy.wait_send()

    width = min(512, order)
    w_rows = lax.broadcasted_iota(jnp.int32, (BLOCK, width), 0)

    def slot_line(t):
        line = jnp.zeros((1, 128), jnp.int32)
        for r in range(8):
            line = jnp.where(lane1 // vectors == r, slots[8 * t + r] * vectors + lane1 % vectors, line)
        return line

    def one_hot(i, j):
        line = jnp.concatenate([slot_line(j * (width // 128) + t) for t in range(width // 128)], axis=1)
        return jnp.where(w_rows + i * BLOCK == line, 1.0, 0.0)

    if blocks <= 4:
        for i in range(blocks):
            right = one_hot(i, 0)
            if i:
                at = slice((i % per_slab) * BLOCK, (i % per_slab + 1) * BLOCK)
                right = right - dot(full[i // per_slab, at, 0 : i * BLOCK], sol_mat[0 : i * BLOCK])
            sol_mat[i * BLOCK : (i + 1) * BLOCK] = dot(inv[i], right)
    else:
        def wipe(i, _):
            sol_mat[pl.ds(pl.multiple_of(i * 8, 8), 8), :] = jnp.zeros((8, order), f32)
            return 0

        lax.fori_loop(0, order // 8, wipe, 0)

        def substitute(i, _):
            at = pl.ds(pl.multiple_of((i % per_slab) * BLOCK, BLOCK), BLOCK)
            for j in range(order // width):
                col = slice(j * width, (j + 1) * width)
                right = one_hot(i, j) - dot(full[i // per_slab, at, :], sol_mat[:, col])
                sol_mat[pl.ds(pl.multiple_of(i * BLOCK, BLOCK), BLOCK), col] = dot(inv[i], right)
            return 0

        lax.fori_loop(0, blocks, substitute, 0)

    mine = pl.ds(pl.multiple_of((me // 8) * 128, 128), 128)

    def turn(i, _):
        at = pl.ds(pl.multiple_of(i * BLOCK, BLOCK), BLOCK)
        turned[:, at] = sol_mat[at, mine].T
        return 0

    lax.fori_loop(0, blocks, turn, 0)
    own_rows = pl.ds(pl.multiple_of(base, 8), vectors)

    def form(j, _):
        col = pl.ds(pl.multiple_of(j * width, width), width)
        krows[:, col] = dot(turned[own_rows, :], sol_mat[:, col])
        return 0

    lax.fori_loop(0, order // width, form, 0)

    def coarse():
        y = jnp.zeros((vectors, 128), f32)
        for t in range(order // 128):
            y = y + krows[:, t * 128 : (t + 1) * 128] * gres[t]
        y = jnp.broadcast_to(jnp.sum(y, axis=1, keepdims=True), (vectors, 128))
        spread = [jnp.broadcast_to(y[k : k + 1], (8, 128)) for k in range(vectors)]

        def correct(x, _):
            for c in range(3):
                for t in range(0, cy, 8):
                    acc = spread[0] * defl[0, c, x, t : t + 8]
                    for k in range(1, vectors):
                        acc = acc + spread[k] * defl[k, c, x, t : t + 8]
                    cor[c, W + x, W + t : W + t + 8] = acc
            return 0

        lax.fori_loop(0, cx, correct, 0)

    lines, _, _ = collect(0)
    for t in range(n // 8):
        gres[t] = lines[t]
        gdir[t] = jnp.zeros((1, 128), f32)
    coarse()
    send_halo(*thin)
    take_halo(*halo_z(0))
    take_halo(*halo_m)
    rows = lax.broadcasted_iota(jnp.int32, (pitch, 128), 0)
    y_ok = ((rows >= W) | (gy > 0)) & ((rows < W + cy) | (gy < ny - 1)) & (rows < cy + 2 * W)

    def settle(x, acc):
        x_ok = ((x >= W) | (gx > 0)) & ((x < W + cx) | (gx < nx - 1))
        keep = jnp.where(x_ok, 1.0, 0.0)
        v = jnp.where(y_ok, 0.6 / (mext[0, x] + 2.75), 0.0) * keep
        cext[x] = v
        cquarter[x] = 0.25 * v
        out = [gathered(v[0:tall], x, acc[3])]
        new = []
        for c in range(3):
            f = zext[0, c, x]
            rext[c, x] = f
            idir[c, x] = jnp.zeros((pitch, 128), f32)
            u = v[0:tall] * f[0:tall]
            ua[c, x, 0:tall] = u
            new.append(gathered(u, x, acc[c]))
        return tuple(new) + tuple(out)

    acc = planes(0, ex, settle, nothing + (nothing[0],), 2)
    cpack[0:tall] = acc[3]
    send_columns(0, 0, acc[0:3])

    def own_clear(x, _):
        for c in range(3):
            sol[c, x] = jnp.zeros((cy, 128), f32)
            direc[c, x] = jnp.zeros((cy, 128), f32)
        return 0

    lax.fori_loop(0, cx, own_clear, 0)

    def iterate(it, carry):
        gamma_prior, step_prior = carry
        slot = (it + 1) % 2
        sweep(ua, ub, 2)
        take_columns(0, 1, True)
        acc = mend(ub, 2, None)
        send_columns(1, 1, acc)
        sweep(ub, uz, 1)
        take_columns(1, 2, True)
        take_halo(*thin)
        acc = mend(uz, 1, cor)
        send_columns(2, 2, acc)

        def image(x, _):
            for t in range(0, cy, 8):
                here, off = stencil(uz, x, W + t)
                diag = mext[0, x, W + t : W + t + 8] + 2.75
                for c in range(3):
                    zext[slot, c, x, W + t : W + t + 8] = diag * here[c] - 0.25 * off[c]
            return 0

        planes(W, W + cx, image, 0, 8)
        take_columns(2, 3, False)

        def finish(x, carry):
            gam, ene, acc = carry[0], carry[1], carry[2:]
            values = []
            for c in range(3):
                f = pltpu.roll(fix[c, W : W + cy], 127 - 2 * W - 2 * x, 1)
                a = zext[slot, c, W + x, W : W + cy] - jnp.where(rim_own, f, 0.0)
                zext[slot, c, W + x, W : W + cy] = a
                z = uz[c, W + x, W : W + cy]
                gam = gam + rext[c, W + x, W : W + cy] * z
                ene = ene + z * a
                values.append(a)
            return (gam, ene) + tuple(restrict(x, values, acc))

        blank = jnp.zeros((cy, 128), f32)
        carry = planes(0, cx, finish, (blank, blank) + clean, 4)
        gam = jnp.sum(jnp.sum(carry[0], axis=0, keepdims=True), axis=1, keepdims=True)
        ene = jnp.sum(jnp.sum(carry[1], axis=0, keepdims=True), axis=1, keepdims=True)
        push(slot, carry[2:], gam, ene)

        @pl.when(it < ITERS - 1)
        def _():
            send_halo(*halo_z(slot))

        lines, gamma, energy = collect(slot)
        momentum = jnp.where(it == 0, 0.0, gamma / gamma_prior)
        step = gamma / (energy - momentum * gamma / step_prior)

        @pl.when(it < ITERS - 1)
        def _():
            for t in range(n // 8):
                image_line = lines[t] + momentum * gdir[t]
                gdir[t] = image_line
                gres[t] = gres[t] - step * image_line
            coarse()
            send_halo(*thin)
            take_halo(*halo_z(slot))

            def update(x, acc):
                out = []
                for c in range(3):
                    image_dir = zext[slot, c, x, 0:tall] + momentum * idir[c, x, 0:tall]
                    idir[c, x, 0:tall] = image_dir
                    r = rext[c, x, 0:tall] - step * image_dir
                    rext[c, x, 0:tall] = r
                    u = cext[x, 0:tall] * r
                    ua[c, x, 0:tall] = u
                    out.append(gathered(u, x, acc[c]))
                return tuple(out)

            acc = planes(0, ex, update, nothing, 11)
            send_columns(0, 0, acc)

        def advance(x, _):
            for c in range(3):
                d = uz[c, W + x, W : W + cy] + momentum * direc[c, x]
                direc[c, x] = d
                sol[c, x] = sol[c, x] + step * d
            return 0

        lax.fori_loop(0, cx, advance, 0)

        @pl.when(it == ITERS - 1)
        def _():
            def give(x, _):
                for c in range(3):
                    image_dir = zext[slot, c, W + x, W : W + cy] + momentum * idir[c, W + x, W : W + cy]
                    res[c, x] = rext[c, W + x, W : W + cy] - step * image_dir
                return 0

            lax.fori_loop(0, cx, give, 0)

        return gamma, step

    one = jnp.ones((1, 1), f32)
    lax.fori_loop(0, ITERS, iterate, (one, one))


def hand_out(whole, *refs):
    outs, sems = refs[:-1], refs[-1]
    copies = [pltpu.make_async_copy(whole.at[i], out, sems.at[i]) for i, out in enumerate(outs)]
    for copy in copies:
        copy.start()
    for copy in copies:
        copy.wait()


def solution(mesh):
    nx, ny, nz = mesh.shape["gx"], mesh.shape["gy"], mesh.shape["gz"]

    def body(forces, mass_shift, deflation, coarse_factor, coarse_slot):
        vectors = deflation.shape[0]
        cx, cy = forces.shape[1], forces.shape[2]
        order = coarse_factor.shape[1]
        slab = coarse_factor.shape[0]
        n = nx * ny * nz
        ex, pitch = cx + 2 * W, up8(up8(cy + 2 * W) + W)
        f32 = jnp.float32
        vm = lambda *shape: pltpu.VMEM(shape, f32)
        field = (3, ex, pitch, 128)
        dma = pltpu.SemaphoreType.DMA
        peers = max(nz - 1, 1)
        room = 66 * 1000 * 1000
        whole = pl.pallas_call(
            functools.partial(kernel, (nx, ny, nz, cx, cy, vectors, order)),
            out_shape=jax.ShapeDtypeStruct((3, *forces.shape), f32),
            in_specs=[pl.BlockSpec(memory_space=pl.ANY)] * 5,
            out_specs=pl.BlockSpec(memory_space=pltpu.VMEM),
            scratch_shapes=[
                vm(2, *field), vm(*field), vm(*field), vm(ex, pitch, 128), vm(ex, pitch, 128),
                vm(1, ex, pitch, 128), vm(*field), vm(*field), vm(*field), vm(*field),
                vm(3, 3, pitch, 128), vm(3, 2, 3, pitch, 128), vm(3, pitch, 128), vm(3, pitch, 128),
                vm(pitch, 128), vm(*deflation.shape),
                vm(nz, slab, order), vm(order // BLOCK, BLOCK, BLOCK), vm(order, order),
                vm(BLOCK, order), vm(vectors, order),
                vm(2, 8, 128), vm(2, n, 128), vm(n // 8, 1, 128), vm(n // 8, 1, 128),
                pltpu.SMEM(coarse_slot.shape, jnp.int32),
                dma((8,)), dma((2, 8)), dma((8,)), dma((8,)), dma((8,)), dma((8,)),
                dma((3, 2)), dma((3, 2)), dma((2,)), dma((2,)),
                dma((peers,)), dma((peers,)), dma((peers,)), dma((peers,)), dma((5,)),
            ],
            compiler_params=pltpu.CompilerParams(
                collective_id=0, has_side_effects=True, vmem_limit_bytes=room
            ),
        )(forces, mass_shift, deflation, coarse_factor, coarse_slot)
        return pl.pallas_call(
            hand_out,
            out_shape=[jax.ShapeDtypeStruct(forces.shape, f32)] * 3,
            in_specs=[pl.BlockSpec(memory_space=pltpu.VMEM)],
            out_specs=[pl.BlockSpec(memory_space=pl.ANY)] * 3,
            scratch_shapes=[dma((3,))],
            compiler_params=pltpu.CompilerParams(vmem_limit_bytes=4 * 1000 * 1000),
        )(whole)

    return jax.shard_map(
        body,
        mesh=mesh,
        in_specs=(
            P(None, "gx", "gy", "gz"),
            P("gx", "gy", "gz"),
            P(None, None, "gx", "gy", "gz"),
            P("gz", None),
            P(),
        ),
        out_specs=(P(None, "gx", "gy", "gz"), P(None, "gx", "gy", "gz"), P(None, "gx", "gy", "gz")),
        check_vma=False,
    )
```
